256 devices in a mesh: hst: 16 (over z, core), local: 16 (over y, x).
Axes of the slice: x: 4, y: 4, z: 8, core: 2. Of those that a mesh axis runs over, the one named last changes fastest.
Arguments:
- teacher_logits: bfloat16 [512, 24, 32000], P(('hst', 'local')), may hold values from -360 to 450
- sample_ids: int32 [512, 24], P(('hst', 'local')), may hold values from 0 to 23, as said below
- client_counts: int32 [512], P(('hst', 'local')), may hold values from 1 to 999
- student_hidden: bfloat16 [24, 4096], replicated, may hold values from -60 to 60
- student_weight: bfloat16 [4096, 32000], P(None, ('hst', 'local')), may hold values from -0.0625 to 0.0625
Outputs:
- grad_weight: bfloat16 [4096, 32000], P(None, ('hst', 'local'))
- grad_hidden: float32 [24, 4096], P(None, ('hst', 'local'))
The draws below stay inside these ranges and needn't reach their ends.
Inputs may be any that keep to these rules, and one draw needn't show every extreme that they name: `sample_ids`: for each client the row is a permutation of 0 to 23.
All inputs are finite; a program needn't handle non-finite values.
Results may differ from the reference program's by a relative error of at most 0.0056.
Values sent between devices are 32-bit elements; how exact they have to be, the bound alone decides.
A program may use at most 64 MiB of HBM per device.

```python
import jax
import jax.numpy as jnp
from jax import lax

VOCABULARY = 32000
MODEL_WIDTH = 4096
SAMPLES = 24
CLIENTS = 512


def sample_order(key):
    client_keys = jax.random.split(jax.random.fold_in(key, 11), CLIENTS)

    def permute(single):
        return jax.random.permutation(single, SAMPLES).astype(jnp.int32)
    return jax.vmap(permute)(client_keys)


def draw_sample_ids(key, part):
    return sample_order(key)


def draw_teacher_logits(key, part):
    orders = sample_order(key)
    base_key, pair_key = jax.random.split(jax.random.fold_in(key, 23), 2)
    block = VOCABULARY // CLIENTS
    pairing = jax.random.permutation(pair_key, CLIENTS).astype(jnp.int32)
    columns = jnp.arange(VOCABULARY, dtype=jnp.int32)
    client_keys = jax.random.split(base_key, CLIENTS)
    clients = jnp.arange(CLIENTS, dtype=jnp.int32)

    def one_client(item):
        client, single, order = item
        values = 3.0 * jnp.clip(jax.random.normal(single, (SAMPLES, VOCABULARY), jnp.float32), -4.0, 4.0)
        spiked = jnp.where(columns // block == pairing[client], 30.0, 1.0)
        values = values * spiked[None, :]
        return values[order].astype(jnp.bfloat16)
    return lax.map(one_client, (clients, client_keys, orders))


def student_pair(key):
    weight_key, hidden_key = jax.random.split(jax.random.fold_in(key, 37), 2)
    weight = jnp.clip(jax.random.normal(weight_key, (MODEL_WIDTH, VOCABULARY), jnp.float32), -4.0, 4.0) * 0.015625
    hidden = 3.0 * jnp.clip(jax.random.normal(hidden_key, (SAMPLES, MODEL_WIDTH), jnp.float32), -4.0, 4.0)
    return (weight, hidden)


def draw_student_weight(key, part):
    weight, hidden = student_pair(key)
    return weight.astype(jnp.bfloat16)


def draw_student_hidden(key, part):
    weight, hidden = student_pair(key)
    return hidden.astype(jnp.bfloat16)


def place_ends(entries, stream_key, low, high):
    longest = entries.shape.index(max(entries.shape))
    spots = []
    for shift in (0, 1):
        where = [jax.random.randint(jax.random.fold_in(stream_key, axis), (), 0, length) for axis, length in enumerate(entries.shape)]
        where[longest] = (where[longest] + shift) % entries.shape[longest]
        spots.append(tuple(where))
    return entries.at[spots[0]].set(low).at[spots[1]].set(high)


def setup_inputs(seed: int = 0) -> dict:
    keys = jax.random.split(jax.random.key(seed), 6)
    teacher_logits = draw_teacher_logits(jax.random.fold_in(keys[5], 71), 0)
    sample_ids = draw_sample_ids(jax.random.fold_in(keys[5], 71), 0)
    client_counts = place_ends(jax.random.randint(keys[2], (CLIENTS,), 1, 1000), jax.random.fold_in(keys[2], 1), 1, 999).astype(jnp.int32)
    student_hidden = draw_student_hidden(jax.random.fold_in(keys[5], 71), 0)
    student_weight = draw_student_weight(jax.random.fold_in(keys[5], 71), 0)
    return dict(teacher_logits=teacher_logits, sample_ids=sample_ids, client_counts=client_counts, student_hidden=student_hidden, student_weight=student_weight)


def reference(teacher_logits, sample_ids, client_counts, student_hidden, student_weight):
    places = jnp.arange(SAMPLES, dtype=jnp.int32)

    def accumulate(carry, item):
        logits, order, count = item
        selector = (order[None, :] == places[:, None]).astype(logits.dtype)
        aligned = jnp.dot(selector, logits, preferred_element_type=jnp.float32)
        return carry + count.astype(jnp.float32) * aligned, None

    start = jnp.zeros((SAMPLES, VOCABULARY), jnp.float32)
    weighted, _ = lax.scan(accumulate, start, (teacher_logits, sample_ids, client_counts))
    count_total = jnp.sum(client_counts.astype(jnp.float32))
    ensemble = weighted / count_total
    teacher_prob = jax.nn.softmax(ensemble, axis=1)
    student_logits = jnp.dot(student_hidden, student_weight, preferred_element_type=jnp.float32)
    student_prob = jax.nn.softmax(student_logits, axis=1)
    grad_logits = ((32768.0 / SAMPLES) * (student_prob - teacher_prob)).astype(jnp.bfloat16)
    grad_weight = jnp.dot(student_hidden.T, grad_logits, preferred_element_type=jnp.float32).astype(jnp.bfloat16)
    grad_hidden = jnp.dot(grad_logits, student_weight.T, preferred_element_type=jnp.float32)
    return grad_weight, grad_hidden
```

```python
import jax
import jax.numpy as jnp
from jax import lax
from jax.experimental import pallas as pl
from jax.experimental.pallas import tpu as pltpu
from jax.sharding import PartitionSpec as P

MESH = pl.DeviceIdType.MESH
F32 = jnp.float32
BF16 = jnp.bfloat16
SAMPLES = 24
VOCAB = 32000
WIDTH = 4096
SLICE = 125
LANES = 128
SCALE = 32768.0 / SAMPLES
OFFSETS = (2, 1, 3, 0)
PARTS = 5
PART_COLUMNS = VOCAB // PARTS
STEP_COLUMNS = 1280
STEPS = PART_COLUMNS // STEP_COLUMNS
LOW = -3.0e38


def remote(src, dst, send_sem, recv_sem, hst, loc):
    return pltpu.make_async_remote_copy(
        src_ref=src,
        dst_ref=dst,
        send_sem=send_sem,
        recv_sem=recv_sem,
        device_id={"hst": hst, "local": loc},
        device_id_type=MESH,
    )


def lane_index(rows):
    return lax.broadcasted_iota(jnp.int32, (rows, LANES), 1)


def masked_stats(values):
    valid = lane_index(SAMPLES) < SLICE
    top = jnp.max(jnp.where(valid, values, LOW), axis=1, keepdims=True)
    weights = jnp.where(valid, jnp.exp(values - top), 0.0)
    return top, jnp.sum(weights, axis=1, keepdims=True), weights


def packed_stats(top, total):
    lane = lane_index(8)
    tile = jnp.zeros((8, LANES), F32)
    for r in range(3):
        tile = jnp.where((lane >= 16 * r) & (lane < 16 * r + 16), top[8 * r : 8 * r + 8], tile)
        low = 48 + 16 * r
        tile = jnp.where((lane >= low) & (lane < low + 16), total[8 * r : 8 * r + 8], tile)
    return tile


def split_two(weights):
    high = weights.astype(BF16)
    low = (weights - high.astype(F32)).astype(BF16)
    return jnp.concatenate([high, low], axis=0)[:, :SLICE]


def partial_blocks(both, w_perm, core, out, stats):
    rows = w_perm[core].reshape(WIDTH // 2, SLICE)
    product = lax.dot_general(both, rows, (((1,), (1,)), ((), ())), preferred_element_type=F32)
    product = product[:SAMPLES] + product[SAMPLES:]
    for b in range(16):
        out[b, 0:SAMPLES, :] = product[:, LANES * b : LANES * (b + 1)]
        out[b, SAMPLES:32, :] = stats


def factors(stat, joined):
    scale = jnp.exp(stat - joined)
    return scale, [scale[:, 16 * r : 16 * r + 1] for r in range(3)]


def join_cores(own, came):
    mine, theirs = own[0, SAMPLES:32, :], came[0, SAMPLES:32, :]
    joined = jnp.maximum(mine, theirs)
    f_mine, mine_rows = factors(mine, joined)
    f_theirs, their_rows = factors(theirs, joined)
    total = mine * pltpu.roll(f_mine, 48, 1) + theirs * pltpu.roll(f_theirs, 48, 1)
    stats = jnp.where(lane_index(8) < 48, joined, total)
    for b in range(16):
        for r in range(3):
            rows = slice(8 * r, 8 * r + 8)
            own[b, rows, :] = own[b, rows, :] * mine_rows[r] + came[b, rows, :] * their_rows[r]
        own[b, SAMPLES:32, :] = stats


def join_plane(own, here, came):
    mine = own[here]
    stats = [mine[SAMPLES:32]] + [came[k, SAMPLES:32, :] for k in range(1, 16)]
    joined = stats[0]
    for stat in stats[1:]:
        joined = jnp.maximum(joined, stat)
    total = jnp.zeros((8, LANES), F32)
    sums = [jnp.zeros((8, LANES), F32) for _ in range(3)]
    for k in range(16):
        scale, rows = factors(stats[k], joined)
        total = total + stats[k] * pltpu.roll(scale, 48, 1)
        for r in range(3):
            block = mine[8 * r : 8 * r + 8] if k == 0 else came[k, 8 * r : 8 * r + 8, :]
            sums[r] = sums[r] + block * rows[r]
    tops = [joined[:, 16 * r : 16 * r + 1] for r in range(3)]
    totals = [total[:, 48 + 16 * r : 49 + 16 * r] for r in range(3)]
    return sums, tops, totals


def kernel(
    counts, ids, logits_hbm, hidden_hbm, weight_hbm, perm_hbm,
    grad_ref, hidden_out,
    x_in, local, hidden, weight, w_perm,
    to_core, own, from_core,
    fwd1, got1, second, fwd2, got2, third, from_z,
    t_own, t_to, t_from, t_plane, s_own, s_to, s_from, s_plane,
    z_to, z_from, teacher, student,
    load_sems, core_send, core_recv, ring_send, ring_recv,
    z_send, z_recv, side_send, side_recv, plane_send, plane_recv, last_send, last_recv,
):
    hst, loc = lax.axis_index("hst"), lax.axis_index("local")
    z, c = hst // 2, hst % 2
    y, x = loc // 4, loc % 4
    other = z * 2 + (1 - c)

    barrier = pltpu.get_barrier_semaphore()

    def greet(to_hst, to_loc):
        pl.semaphore_signal(
            barrier, inc=1, device_id={"hst": to_hst, "local": to_loc}, device_id_type=MESH
        )

    greet(other, loc)
    for k in range(1, 16):
        greet(hst, ((y + k // 4) % 4) * 4 + (x + k % 4) % 4)
    for k in range(1, 8):
        greet(((z + k) % 8) * 2 + c, loc)

    loads = [
        pltpu.make_async_copy(
            logits_hbm.at[:, pl.ds(k * PART_COLUMNS, PART_COLUMNS)],
            x_in.at[:, pl.ds(k * PART_COLUMNS, PART_COLUMNS)],
            load_sems.at[k],
        )
        for k in range(PARTS)
    ]
    late = [
        pltpu.make_async_copy(hidden_hbm, hidden, load_sems.at[PARTS]),
        pltpu.make_async_copy(weight_hbm, weight, load_sems.at[PARTS + 1]),
    ]
    for a in range(8):
        for b in range(2):
            late.append(
                pltpu.make_async_copy(
                    perm_hbm.at[a, b], w_perm.at[b, :, :, a], load_sems.at[PARTS + 2 + 2 * a + b]
                )
            )
    for load in loads + late:
        load.start()

    place = lax.broadcasted_iota(jnp.int32, (48, SAMPLES), 0)
    first = (ids[0:1, :] == place).astype(F32)
    second_half = (ids[1:2, :] == place - SAMPLES).astype(F32)
    selector = jnp.concatenate([first, second_half], axis=1).astype(BF16)
    count0 = counts[0].astype(F32)
    count1 = counts[1].astype(F32)
    count_sum = count0 + count1

    for k in range(PARTS):
        loads[k].wait()

        def multiply(i, carry, k=k):
            at = pl.multiple_of(k * PART_COLUMNS + i * STEP_COLUMNS, LANES)
            aligned = jnp.dot(
                selector, x_in[:, pl.ds(at, STEP_COLUMNS)], preferred_element_type=F32
            )
            both = count0 * aligned[:SAMPLES] + count1 * aligned[SAMPLES:]
            tile = (k * PART_COLUMNS + i * STEP_COLUMNS) // LANES
            for j in range(STEP_COLUMNS // LANES):
                local[tile + j] = both[:, LANES * j : LANES * (j + 1)]
            return carry

        lax.fori_loop(0, STEPS, multiply, 0)

    pl.semaphore_wait(barrier, 23)

    lane = lane_index(SAMPLES)

    def sliced(device):
        start = device * SLICE
        tile, shift = start // LANES, start % LANES
        back = (LANES - shift) % LANES
        low = pltpu.roll(local[tile], back, 1)
        high = pltpu.roll(local[tile + 1], back, 1)
        block = jnp.where(lane < LANES - shift, low, high)
        return jnp.where(lane < SLICE, block, count_sum)

    core_copies = []
    for k in range(4):
        def cut(i, carry, k=k):
            color, half, kk, zlo = i // 16, (i // 8) % 2, (i // 2) % 4, i % 2
            along = (x * (1 - color) + y * color + OFFSETS[k]) % 4
            across = (y * (1 - color) + x * color + kk) % 4
            to_x = along * (1 - color) + across * color
            to_y = across * (1 - color) + along * color
            to_z = color * 4 + half * 2 + zlo
            base = to_z * 32 + to_y * 4 + to_x
            to_core[32 * k + i] = sliced(base + 16 * (1 - c))
            own[32 * k + i] = sliced(base + 16 * c)
            return carry

        lax.fori_loop(0, 32, cut, 0, unroll=2)
        part = pl.ds(32 * k, 32)
        copy = remote(
            to_core.at[part], from_core.at[part], core_send.at[k], core_recv.at[k], other, loc
        )
        copy.start()
        core_copies.append(copy)

    x_next, x_back = y * 4 + (x + 1) % 4, y * 4 + (x + 3) % 4
    y_next, y_back = ((y + 1) % 4) * 4 + x, ((y + 3) % 4) * 4 + x

    def add_range(dst, at, src, src_at, count):
        def add(i, carry):
            dst[at + i] = dst[at + i] + src[src_at + i]
            return carry

        lax.fori_loop(0, count, add, 0, unroll=2)

    sent = list(core_copies)

    def start(copy):
        copy.start()
        sent.append(copy)
        return copy

    ways1 = ((x_next, x_back), (y_next, y_back))
    forwards1, direct1, relayed1 = {}, {}, {}

    def sem(stage, color, kind):
        return stage * 12 + color * 6 + kind

    def ring(stage, color, kind, src, dst, to):
        n = sem(stage, color, kind)
        return start(remote(src, dst, ring_send.at[n], ring_recv.at[n], hst, to))

    core_copies[0].wait_recv()
    add_range(own, 0, from_core, 0, 32)
    for color in range(2):
        ahead, behind = ways1[color]
        base = 16 * color
        for half, to in ((0, ahead), (1, behind)):
            forwards1[color, half] = ring(
                0, color, half, own.at[pl.ds(base + 8 * half, 8)], fwd1.at[2 * color + half], to
            )
    for k, half in ((1, 1), (2, 0)):
        core_copies[k].wait_recv()
        add_range(own, 32 * k, from_core, 32 * k, 32)
        for color in range(2):
            to = ways1[color][k - 1]
            direct1[color, k] = ring(
                0, color, 1 + k, own.at[pl.ds(32 * k + 16 * color + 8 * half, 8)],
                got1.at[2 * color + k - 1, pl.ds(8 * half, 8)], to,
            )
    core_copies[3].wait_recv()
    add_range(own, 96, from_core, 96, 32)
    for k, half in ((1, 0), (2, 1)):
        for color in range(2):
            forwards1[color, half].wait_recv()
            at = 32 * k + 16 * color + 8 * half
            for i in range(8):
                own[at + i] = own[at + i] + fwd1[2 * color + half, i]
            relayed1[color, k] = ring(
                0, color, 3 + k, own.at[pl.ds(at, 8)],
                got1.at[2 * color + k - 1, pl.ds(8 * half, 8)], ways1[color][k - 1],
            )

    for load in late:
        load.wait()
    values = jnp.dot(hidden[...], weight[...], preferred_element_type=F32)
    values = jnp.concatenate([values, jnp.zeros((SAMPLES, 3), F32)], axis=1)
    student[...] = values
    top, total, weights = masked_stats(values)
    both = split_two(weights)
    stats = packed_stats(top, total)
    partial_blocks(both, w_perm, 1 - c, s_to, stats)
    side_s = start(remote(s_to, s_from, side_send.at[0], side_recv.at[0], other, loc))
    partial_blocks(both, w_perm, c, s_own, stats)
    side_s.wait_recv()
    join_cores(s_own, s_from)

    for color in range(2):
        for k in (1, 2):
            direct1[color, k].wait_recv()
            relayed1[color, k].wait_recv()
        for i in range(16):
            second[color, i] = (
                own[96 + 16 * color + i] + got1[2 * color, i] + got1[2 * color + 1, i]
            )
    ways2 = ((y_next, y_back), (x_next, x_back))
    forwards2, direct2, relayed2 = {}, {}, {}
    for color in range(2):
        for half in range(2):
            forwards2[color, half] = ring(
                1, color, half, second.at[color, pl.ds(8 * half + 4, 2)],
                fwd2.at[2 * color + half], ways2[color][half],
            )
        for k, half, kk in ((1, 1, 1), (2, 0, 3)):
            direct2[color, k] = ring(
                1, color, 1 + k, second.at[color, pl.ds(8 * half + 2 * kk, 2)],
                got2.at[2 * color + k - 1, pl.ds(2 * half, 2)], ways2[color][k - 1],
            )
    for color in range(2):
        for k, half, kk in ((1, 0, 1), (2, 1, 3)):
            forwards2[color, half].wait_recv()
            at = 8 * half + 2 * kk
            for i in range(2):
                second[color, at + i] = second[color, at + i] + fwd2[2 * color + half, i]
            relayed2[color, k] = ring(
                1, color, 3 + k, second.at[color, pl.ds(at, 2)],
                got2.at[2 * color + k - 1, pl.ds(2 * half, 2)], ways2[color][k - 1],
            )
    for color in range(2):
        for k in (1, 2):
            direct2[color, k].wait_recv()
            relayed2[color, k].wait_recv()
        for half in range(2):
            for i in range(2):
                third[4 * color + 2 * half + i] = (
                    second[color, 8 * half + i]
                    + got2[2 * color, 2 * half + i]
                    + got2[2 * color + 1, 2 * half + i]
                )

    z_copies = []
    for k in (4, 3, 5, 2, 6, 1, 7):
        to_z = (z + k) % 8
        z_copies.append(
            start(remote(third.at[to_z], from_z.at[k], z_send.at[k], z_recv.at[k], to_z * 2 + c, loc))
        )

    def plane(src, dst, which):
        copies = []
        for k in range(1, 16):
            to = ((y + k // 4) % 4) * 4 + (x + k % 4) % 4
            copies.append(
                start(
                    remote(
                        src.at[to], dst.at[k], plane_send.at[16 * which + k],
                        plane_recv.at[16 * which + k], hst, to,
                    )
                )
            )
        return copies

    student_plane = plane(s_own, s_plane, 0)
    for copy in z_copies:
        copy.wait_recv()
    summed = third[z]
    for k in range(1, 8):
        summed = summed + from_z[k]

    ensemble = summed / summed[:, SLICE : SLICE + 1]
    teacher[...] = ensemble
    top, total, weights = masked_stats(ensemble)
    both = split_two(weights)
    stats = packed_stats(top, total)
    partial_blocks(both, w_perm, 1 - c, t_to, stats)
    side_t = start(remote(t_to, t_from, side_send.at[1], side_recv.at[1], other, loc))
    partial_blocks(both, w_perm, c, t_own, stats)
    side_t.wait_recv()
    join_cores(t_own, t_from)
    teacher_plane = plane(t_own, t_plane, 1)

    for copy in student_plane:
        copy.wait_recv()
    s_sums, s_tops, s_totals = join_plane(s_own, loc, s_plane)
    lane8 = lane_index(8)

    def spread(sums, tops, totals, base, tile, tops_tile):
        for r in range(3):
            low = base + 20 * r
            inside = (lane8 >= low) & (lane8 < low + 16)
            ending = (lane8 >= low + 16) & (lane8 < low + 20)
            for k in range(8):
                moved = pltpu.roll(sums[r], (low - 16 * k) % LANES, 1)
                tile[k] = jnp.where(ending, totals[r], jnp.where(inside, moved, tile[k]))
            tops_tile = jnp.where(inside | ending, tops[r], tops_tile)
        return tops_tile

    tiles = [jnp.zeros((8, LANES), F32) for _ in range(8)]
    tops_tile = spread(s_sums, s_tops, s_totals, 60, tiles, jnp.zeros((8, LANES), F32))
    for copy in teacher_plane:
        copy.wait_recv()
    t_sums, t_tops, t_totals = join_plane(t_own, loc, t_plane)
    tops_tile = spread(t_sums, t_tops, t_totals, 0, tiles, tops_tile)
    for k in range(8):
        z_to[k, 0:8, :] = tiles[k]
        z_to[k, 8:16, :] = tops_tile
    last_copies = []
    for k in (4, 3, 5, 2, 6, 1, 7):
        to_z = (z + k) % 8
        last_copies.append(
            start(remote(z_to.at[to_z], z_from.at[k], last_send.at[k], last_recv.at[k], to_z * 2 + c, loc))
        )
    for copy in last_copies:
        copy.wait_recv()
    mine = z_to[z]
    pieces = [mine] + [z_from[k] for k in range(1, 8)]
    joined = pieces[0][8:16]
    for piece in pieces[1:]:
        joined = jnp.maximum(joined, piece[8:16])
    sums = jnp.zeros((8, LANES), F32)
    for piece in pieces:
        sums = sums + piece[0:8] * jnp.exp(piece[8:16] - joined)

    for r in range(3):
        t_low, s_low = 20 * r, 60 + 20 * r
        t_top, s_top = joined[:, t_low : t_low + 1], joined[:, s_low : s_low + 1]
        t_total = sums[:, t_low + 16 : t_low + 17]
        s_total = sums[:, s_low + 16 : s_low + 17]
        rows = slice(8 * r, 8 * r + 8)
        t_part = pltpu.roll(sums, (LANES - t_low) % LANES, 1) / t_total
        s_part = pltpu.roll(sums, (LANES - s_low) % LANES, 1) / s_total
        hidden_out[rows, :] = (SCALE * (s_part - t_part))[:, :16]
        s_prob = jnp.exp(student[rows, :] - s_top) / s_total
        t_prob = jnp.exp(teacher[rows, :] - t_top) / t_total
        grad_ref[rows, :] = (SCALE * (s_prob - t_prob))[:, :SLICE]

    for copy in sent:
        copy.wait_send()


def per_device(teacher_logits, sample_ids, client_counts, student_hidden, student_weight):
    logits = teacher_logits.reshape(2 * SAMPLES, VOCAB)
    perm = student_weight.reshape(8, 2, 4, 4, 16, SLICE)
    any_spec = pl.BlockSpec(memory_space=pltpu.HBM)
    vmem = pl.BlockSpec(memory_space=pltpu.VMEM)
    block = (SAMPLES, LANES)
    tall = (16, 32, LANES)
    dma = pltpu.SemaphoreType.DMA
    grad, grad_hidden = pl.pallas_call(
        kernel,
        out_shape=(
            jax.ShapeDtypeStruct((SAMPLES, SLICE), F32),
            jax.ShapeDtypeStruct((SAMPLES, 16), F32),
        ),
        in_specs=[pl.BlockSpec(memory_space=pltpu.SMEM), vmem] + [any_spec] * 4,
        out_specs=(vmem, vmem),
        scratch_shapes=[
            pltpu.VMEM((2 * SAMPLES, VOCAB), BF16),
            pltpu.VMEM((VOCAB // LANES + 2, *block), F32),
            pltpu.VMEM((SAMPLES, WIDTH), BF16),
            pltpu.VMEM((WIDTH, SLICE), BF16),
            pltpu.VMEM((2, 4, 4, 8, 16, SLICE), BF16),
            pltpu.VMEM((128, *block), F32),
            pltpu.VMEM((128, *block), F32),
            pltpu.VMEM((128, *block), F32),
            pltpu.VMEM((4, 8, *block), F32),
            pltpu.VMEM((4, 16, *block), F32),
            pltpu.VMEM((2, 16, *block), F32),
            pltpu.VMEM((4, 2, *block), F32),
            pltpu.VMEM((4, 4, *block), F32),
            pltpu.VMEM((8, *block), F32),
            pltpu.VMEM((8, *block), F32),
            pltpu.VMEM(tall, F32),
            pltpu.VMEM(tall, F32),
            pltpu.VMEM(tall, F32),
            pltpu.VMEM(tall, F32),
            pltpu.VMEM(tall, F32),
            pltpu.VMEM(tall, F32),
            pltpu.VMEM(tall, F32),
            pltpu.VMEM(tall, F32),
            pltpu.VMEM((8, 16, LANES), F32),
            pltpu.VMEM((8, 16, LANES), F32),
            pltpu.VMEM(block, F32),
            pltpu.VMEM(block, F32),
            dma((PARTS + 18,)),
            dma((4,)),
            dma((4,)),
            dma((24,)),
            dma((24,)),
            dma((8,)),
            dma((8,)),
            dma((2,)),
            dma((2,)),
            dma((32,)),
            dma((32,)),
            dma((8,)),
            dma((8,)),
        ],
        compiler_params=pltpu.CompilerParams(
            collective_id=0, has_side_effects=True, vmem_limit_bytes=48 * 1024 * 1024
        ),
        name="distill",
    )(client_counts, sample_ids, logits, student_hidden, student_weight, perm)
    grad_weight = lax.dot_general(
        student_hidden, grad.astype(BF16), (((0,), (0,)), ((), ())), preferred_element_type=F32
    ).astype(BF16)
    return grad_weight, grad_hidden


def solution(mesh):
    both = ("hst", "local")
    return jax.shard_map(
        per_device,
        mesh=mesh,
        in_specs=(P(both, None, None), P(both, None), P(both), P(), P(None, both)),
        out_specs=(P(None, both), P(None, both)),
        check_vma=False,
    )
```

```python
import jax
import jax.numpy as jnp
from jax import lax
from jax.experimental import pallas as pl
from jax.experimental.pallas import tpu as pltpu
from jax.sharding import PartitionSpec as P

MESH = pl.DeviceIdType.MESH
F32 = jnp.float32
BF16 = jnp.bfloat16
SAMPLES = 24
VOCAB = 32000
WIDTH = 4096
SLICE = 125
LANES = 128
SCALE = 32768.0 / SAMPLES
Z_FAR_FIRST = (4, 3, 5, 2, 6, 1, 7)
FAR_FIRST = (10, 6, 9, 11, 14, 2, 8, 5, 7, 13, 15, 1, 3, 4, 12)
STEP_COLUMNS = 512
STEPS = tuple(-(-min(4000 * (k + 1) + LANES, VOCAB) // STEP_COLUMNS) for k in range(8))
PARTS = 8
WINDOW = 17
LAG = 5
LOW = -3.0e38


def remote(src, dst, send_sem, recv_sem, hst, loc):
    return pltpu.make_async_remote_copy(
        src_ref=src,
        dst_ref=dst,
        send_sem=send_sem,
        recv_sem=recv_sem,
        device_id={"hst": hst, "local": loc},
        device_id_type=MESH,
    )


def lane_index(rows):
    return lax.broadcasted_iota(jnp.int32, (rows, LANES), 1)


def masked_top(values):
    return jnp.max(
        jnp.where(lane_index(SAMPLES) < SLICE, values, LOW), axis=1, keepdims=True
    )


def weighted_product(values, top, rows):
    valid = lane_index(SAMPLES) < SLICE
    weights = jnp.where(valid, jnp.exp(values - top), 0.0)
    product = lax.dot_general(
        split_two(weights), rows, (((1,), (1,)), ((), ())), preferred_element_type=F32
    )
    return jnp.sum(weights, axis=1, keepdims=True), product[:SAMPLES] + product[SAMPLES:]


def packed_stats(top, total):
    lane = lane_index(8)
    tile = jnp.zeros((8, LANES), F32)
    for r in range(3):
        tile = jnp.where((lane >= 16 * r) & (lane < 16 * r + 16), top[8 * r : 8 * r + 8], tile)
        low = 48 + 16 * r
        tile = jnp.where((lane >= low) & (lane < low + 16), total[8 * r : 8 * r + 8], tile)
    return tile


def split_two(weights):
    high = weights.astype(BF16)
    low = (weights - high.astype(F32)).astype(BF16)
    return jnp.concatenate([high, low], axis=0)[:, :SLICE]


def own_part(own, rows, out):
    top = masked_top(own)
    total, product = weighted_product(own, top, rows)
    for b in range(16):
        out[b, 0:SAMPLES, :] = product[:, LANES * b : LANES * (b + 1)]
    return top, total


def other_part(top, total, other, rows, out):
    joined = jnp.maximum(top, masked_top(other))
    more, product = weighted_product(other, joined, rows)
    scale = jnp.exp(top - joined)
    stats = packed_stats(joined, total * scale + more)
    for b in range(16):
        out[b, 0:SAMPLES, :] = (
            out[b, 0:SAMPLES, :] * scale + product[:, LANES * b : LANES * (b + 1)]
        )
        out[b, SAMPLES:32, :] = stats


def factors(stat, joined):
    scale = jnp.exp(stat - joined)
    return scale, [scale[:, 16 * r : 16 * r + 1] for r in range(3)]


def join_plane(own, here, came):
    mine = own[here]
    stats = [mine[SAMPLES:32]] + [came[k, SAMPLES:32, :] for k in range(15)]
    joined = stats[0]
    for stat in stats[1:]:
        joined = jnp.maximum(joined, stat)
    total = jnp.zeros((8, LANES), F32)
    sums = [jnp.zeros((8, LANES), F32) for _ in range(3)]
    for k in range(16):
        scale, rows = factors(stats[k], joined)
        total = total + stats[k] * pltpu.roll(scale, 48, 1)
        for r in range(3):
            block = mine[8 * r : 8 * r + 8] if k == 0 else came[k - 1, 8 * r : 8 * r + 8, :]
            sums[r] = sums[r] + block * rows[r]
    tops = [joined[:, 16 * r : 16 * r + 1] for r in range(3)]
    totals = [total[:, 48 + 16 * r : 49 + 16 * r] for r in range(3)]
    return sums, tops, totals


def kernel(
    counts_hbm, ids_hbm, logits_hbm, hidden_hbm, weight_hbm, perm_hbm,
    grad_ref, hidden_out,
    counts, ids, x_in, local, hidden, weight, w_perm,
    count_to, count_from, blocks, from_core,
    got1, second, got2, third, from_z,
    t_own, t_plane, s_own, s_plane, w_to, w_from, w_other,
    z_to, z_from, teacher, student, s_other, t_other,
    load_sems, core_recv, forward_recv, ring_recv, cross_recv, many_recv, send_sems,
):
    hst, loc = lax.axis_index("hst"), lax.axis_index("local")
    z, c = hst // 2, hst % 2
    y, x = loc // 4, loc % 4
    other = z * 2 + (1 - c)

    early = [
        pltpu.make_async_copy(ids_hbm, ids, load_sems.at[PARTS]),
        pltpu.make_async_copy(counts_hbm, counts, load_sems.at[PARTS + 1]),
    ]
    loads = [
        pltpu.make_async_copy(
            logits_hbm.at[:, pl.ds(low, high - low)], x_in.at[:, pl.ds(low, high - low)],
            load_sems.at[k],
        )
        for k, (low, high) in enumerate(
            (STEP_COLUMNS * ((0,) + STEPS)[k], min(STEP_COLUMNS * STEPS[k], VOCAB))
            for k in range(PARTS)
        )
    ]
    for load in early + loads:
        load.start()

    barrier = pltpu.get_barrier_semaphore()

    def greet(to_hst, to_loc):
        pl.semaphore_signal(
            barrier, inc=1, device_id={"hst": to_hst, "local": to_loc}, device_id_type=MESH
        )

    for k in range(1, 8):
        greet(((z + k) % 8) * 2 + c, loc)
    for k in FAR_FIRST:
        greet(hst, ((y + k // 4) % 4) * 4 + (x + k % 4) % 4)
    greet(other, loc)

    late = [
        pltpu.make_async_copy(hidden_hbm, hidden, load_sems.at[PARTS + 2]),
        pltpu.make_async_copy(weight_hbm, weight, load_sems.at[PARTS + 3]),
    ]
    for load in late:
        load.start()
    for a in range(8):
        for b in range(2):
            pltpu.make_async_copy(
                perm_hbm.at[a, b], w_perm.at[b, :, :, a], load_sems.at[PARTS + 4]
            ).start()
    late.append(pltpu.make_async_copy(w_perm, w_perm, load_sems.at[PARTS + 4]))
    for load in early:
        load.wait()

    place = lax.broadcasted_iota(jnp.int32, (SAMPLES, SAMPLES), 0)
    highs, lows = [], []
    for client in range(2):
        chosen = ids[client : client + 1, :] == place
        high = (counts[client] // 256) * 256
        highs.append(jnp.where(chosen, high.astype(F32), 0.0))
        lows.append(jnp.where(chosen, (counts[client] - high).astype(F32), 0.0))
    one = jnp.concatenate(highs + lows, axis=1)
    none = jnp.zeros_like(one)
    selector = jnp.concatenate(
        [jnp.concatenate([one, none], axis=1), jnp.concatenate([none, one], axis=1)], axis=0
    ).astype(BF16)
    count_sum = (counts[0] + counts[1]).astype(F32)
    count_to[...] = jnp.full((8, LANES), count_sum, F32)
    local[VOCAB // LANES] = jnp.zeros((SAMPLES, LANES), F32)
    lane = lane_index(SAMPLES)
    valid = lane < SLICE

    def multiply(step):
        at = step * STEP_COLUMNS
        groups = min(2, (VOCAB - at) // 256)
        columns = [x_in[:, at + 256 * g : at + 256 * (g + 1)] for g in range(groups)]
        stacked = jnp.concatenate([part for part in columns for _ in range(2)], axis=0)
        sums = jnp.dot(
            selector[: 24 * groups, : 96 * groups], stacked, preferred_element_type=F32
        )
        for g in range(groups):
            tile = at // LANES + 2 * g
            local[tile] = sums[24 * g : 24 * g + 24, :LANES]
            local[tile + 1] = sums[24 * g : 24 * g + 24, LANES:]

    places = []
    for color in range(2):
        for k in range(16):
            dx, dy = (k + 4 - x) % 4, (k // 4 + 4 - y) % 4
            along, across = (dy, dx) if color else (dx, dy)
            places.append(along * 4 + across)

    def first_tile(k, side):
        return (32 * k + 16 * side) * SLICE // LANES

    along_x = [y * 4 + (x + n) % 4 for n in range(4)]
    along_y = [((y + n) % 4) * 4 + x for n in range(4)]
    ways = (along_x, along_y)
    core_copies = []

    def send(src, dst, sem, recv_sem, to_hst, to_loc):
        copy = remote(src, dst, send_sems.at[sem], recv_sem, to_hst, to_loc)
        copy.start()
        return copy

    def arrived(ref, recv_sem):
        pltpu.make_async_copy(ref, ref, recv_sem).wait()

    def pair(k, n, half):
        return blocks.at[pl.ds(16 * k + 4 * n + 2 * half, 2)]

    def landing(k, slot, half):
        return got1.at[k, slot, pl.ds(2 * half, 2)]

    def receive_core(k):
        core_copies[k].wait_recv()
        counted = count_from[0:1, :] + count_sum
        for side_c in range(2):

            @pl.when(c == side_c)
            def cut(side_c=side_c):
                base = first_tile(k, side_c)
                for n in range(16):
                    begin = (32 * k + 16 * side_c + n) * SLICE
                    tile, shift = begin // LANES, begin % LANES
                    block = local[tile] + from_core[k, tile - base]
                    if shift + SLICE > LANES:
                        after = local[tile + 1] + from_core[k, tile + 1 - base]
                        block = jnp.where(lane >= shift, block, after)
                    if shift:
                        block = pltpu.roll(block, LANES - shift, 1)
                    blocks[16 * k + places[16 * (k % 2) + n]] = jnp.where(valid, block, counted)

        way = ways[k % 2]
        for half in range(2):
            send(
                pair(k, 2, half), landing(k, 0, half), 1, forward_recv.at[k], hst,
                way[3 if half else 1],
            )

    def direct(k):
        way = ways[k % 2]
        send(pair(k, 1, 1), landing(k, 1, 1), 1, ring_recv.at[k], hst, way[1])
        send(pair(k, 3, 0), landing(k, 2, 0), 1, ring_recv.at[k], hst, way[3])

    def relay(k):
        way = ways[k % 2]
        arrived(got1.at[k, 0], forward_recv.at[k])
        for half, near in ((0, 1), (1, 3)):
            for n in range(2):
                at = 16 * k + 4 * near + 2 * half + n
                blocks[at] = blocks[at] + got1[k, 0, 2 * half + n]
            send(pair(k, near, half), landing(k, 1 + half, half), 1, ring_recv.at[k], hst, way[near])

    for k in range(8):
        loads[k].wait()
        for step in range(((0,) + STEPS)[k], STEPS[k]):
            multiply(step)
        if k == 0:
            pl.semaphore_wait(barrier, 23)
            count_copy = send(count_to, count_from, 9, many_recv.at[6], other, loc)
        window = c * first_tile(k, 0) + (1 - c) * first_tile(k, 1)
        core_copies.append(
            send(
                local.at[pl.ds(window, WINDOW)], from_core.at[k], 0, core_recv.at[k], other, loc
            )
        )
        if k >= LAG:
            if k == LAG:
                count_copy.wait_recv()
            receive_core(k - LAG)
    for k in range(8 - LAG, 8):
        receive_core(k)
    for k in range(8):
        direct(k)
    for k in range(8):
        relay(k)
    for k in range(8):
        arrived(got1.at[k, pl.ds(1, 2)], ring_recv.at[k])
        for n in range(4):
            second[k % 2, n, k // 2] = blocks[16 * k + n] + (got1[k, 1, n] + got1[k, 2, n])
    for n in (2, 1, 3):
        for color in range(2):
            send(
                second.at[color, n], got2.at[color, n - 1], 2, cross_recv.at[color],
                hst, ways[1 - color][n],
            )
    for load in late:
        load.wait()

    @pl.when(c == 0)
    def widen_second():
        w_to[...] = w_perm[1].reshape(WIDTH // 2, SLICE).astype(F32)

    @pl.when(c == 1)
    def widen_first():
        w_to[...] = w_perm[0].reshape(WIDTH // 2, SLICE).astype(F32)

    w_copy = send(w_to, w_from, 5, many_recv.at[0], other, loc)
    student[:, :SLICE] = jnp.dot(hidden[...], weight[...], preferred_element_type=F32)
    student[:, SLICE:] = jnp.zeros((SAMPLES, LANES - SLICE), F32)
    s_copy = send(student, s_other, 7, many_recv.at[1], other, loc)
    for color in range(2):
        arrived(got2.at[color], cross_recv.at[color])
        for item in range(4):
            third[2 * item + color] = (second[color, 0, item] + got2[color, 0, item]) + (
                got2[color, 1, item] + got2[color, 2, item]
            )
    for k in Z_FAR_FIRST:
        to_z = (z + k) % 8
        send(third.at[to_z], from_z.at[k - 1], 3, many_recv.at[2], to_z * 2 + c, loc)
    w_copy.wait_recv()
    w_other[...] = w_from[...].astype(BF16)
    s_copy.wait_recv()
    own_rows = w_perm[c].reshape(WIDTH // 2, SLICE)
    top, total = own_part(student[...], own_rows, s_own)
    other_part(top, total, s_other[...], w_other[...], s_own)

    def plane(src, dst, sem, recv_sem):
        for k in FAR_FIRST:
            to = ((y + k // 4) % 4) * 4 + (x + k % 4) % 4
            send(src.at[to], dst.at[k - 1], sem, recv_sem, hst, to)

    plane(s_own, s_plane, 6, many_recv.at[3])
    arrived(from_z, many_recv.at[2])
    summed = third[z]
    for k in range(7):
        summed = summed + from_z[k]

    ensemble = summed / summed[:, SLICE : SLICE + 1]
    teacher[...] = ensemble
    t_copy = send(teacher, t_other, 10, many_recv.at[7], other, loc)
    top, total = own_part(ensemble, own_rows, t_own)
    t_copy.wait_recv()
    other_part(top, total, t_other[...], w_other[...], t_own)
    plane(t_own, t_plane, 8, many_recv.at[4])

    arrived(s_plane, many_recv.at[3])
    s_sums, s_tops, s_totals = join_plane(s_own, loc, s_plane)
    lane8 = lane_index(8)

    def spread(sums, tops, totals, base, tile, tops_tile):
        for r in range(3):
            low = base + 20 * r
            inside = (lane8 >= low) & (lane8 < low + 16)
            ending = (lane8 >= low + 16) & (lane8 < low + 20)
            for k in range(8):
                moved = pltpu.roll(sums[r], (low - 16 * k) % LANES, 1)
                tile[k] = jnp.where(ending, totals[r], jnp.where(inside, moved, tile[k]))
            tops_tile = jnp.where(inside | ending, tops[r], tops_tile)
        return tops_tile

    tiles = [jnp.zeros((8, LANES), F32) for _ in range(8)]
    tops_tile = spread(s_sums, s_tops, s_totals, 60, tiles, jnp.zeros((8, LANES), F32))
    arrived(t_plane, many_recv.at[4])
    t_sums, t_tops, t_totals = join_plane(t_own, loc, t_plane)
    tops_tile = spread(t_sums, t_tops, t_totals, 0, tiles, tops_tile)
    for k in range(8):
        z_to[k, 0:8, :] = tiles[k]
        z_to[k, 8:16, :] = tops_tile
    for k in Z_FAR_FIRST:
        to_z = (z + k) % 8
        send(z_to.at[to_z], z_from.at[k - 1], 4, many_recv.at[5], to_z * 2 + c, loc)
    arrived(z_from, many_recv.at[5])
    mine = z_to[z]
    pieces = [mine] + [z_from[k] for k in range(7)]
    joined = pieces[0][8:16]
    for piece in pieces[1:]:
        joined = jnp.maximum(joined, piece[8:16])
    sums = jnp.zeros((8, LANES), F32)
    for piece in pieces:
        sums = sums + piece[0:8] * jnp.exp(piece[8:16] - joined)

    for r in range(3):
        t_low, s_low = 20 * r, 60 + 20 * r
        t_top, s_top = joined[:, t_low : t_low + 1], joined[:, s_low : s_low + 1]
        t_total = sums[:, t_low + 16 : t_low + 17]
        s_total = sums[:, s_low + 16 : s_low + 17]
        rows = slice(8 * r, 8 * r + 8)
        t_part = pltpu.roll(sums, (LANES - t_low) % LANES, 1) / t_total
        s_part = pltpu.roll(sums, (LANES - s_low) % LANES, 1) / s_total
        hidden_out[rows, :] = (SCALE * (s_part - t_part))[:, :16]
        s_prob = jnp.exp(student[rows, :] - s_top) / s_total
        t_prob = jnp.exp(teacher[rows, :] - t_top) / t_total
        grad_ref[rows, :] = (SCALE * (s_prob - t_prob))[:, :SLICE]

    for n, ref in enumerate(
        (from_core, got1, got2, from_z, z_from, w_to, s_plane, student, t_plane, count_to, teacher)
    ):
        arrived(ref, send_sems.at[n])


def finish(grad, grad_hidden, hidden, weight_out, hidden_out, rows, sems):
    rounded = grad[...].astype(BF16)
    size = WIDTH // 4
    copies = []
    for k in range(4):
        part = pl.ds(k * size, size)
        rows[part, :] = lax.dot_general(
            hidden[:, part], rounded, (((0,), (0,)), ((), ())), preferred_element_type=F32
        ).astype(BF16)
        copies.append(pltpu.make_async_copy(rows.at[part], weight_out.at[part], sems.at[k]))
        copies[k].start()
    hidden_out[...] = grad_hidden[...].T
    for copy in copies:
        copy.wait()


def per_device(teacher_logits, sample_ids, client_counts, student_hidden, student_weight):
    logits = teacher_logits.reshape(2 * SAMPLES, VOCAB)
    perm = student_weight.reshape(8, 2, 4, 4, 16, SLICE)
    any_spec = pl.BlockSpec(memory_space=pltpu.HBM)
    vmem = pl.BlockSpec(memory_space=pltpu.VMEM)
    block = (SAMPLES, LANES)
    tall = (16, 32, LANES)
    dma = pltpu.SemaphoreType.DMA
    grad, grad_hidden = pl.pallas_call(
        kernel,
        out_shape=(
            pltpu.VMEM((SAMPLES, SLICE), F32),
            pltpu.VMEM((SAMPLES, 16), F32),
        ),
        in_specs=[any_spec] * 6,
        out_specs=(vmem, vmem),
        scratch_shapes=[
            pltpu.SMEM((2,), jnp.int32),
            pltpu.VMEM((2, SAMPLES), jnp.int32),
            pltpu.VMEM((2 * SAMPLES, VOCAB), BF16),
            pltpu.VMEM((VOCAB // LANES + 2, *block), F32),
            pltpu.VMEM((SAMPLES, WIDTH), BF16),
            pltpu.VMEM((WIDTH, SLICE), BF16),
            pltpu.VMEM((2, 4, 4, 8, 16, SLICE), BF16),
            pltpu.VMEM((8, LANES), F32),
            pltpu.VMEM((8, LANES), F32),
            pltpu.VMEM((128, *block), F32),
            pltpu.VMEM((8, WINDOW, *block), F32),
            pltpu.VMEM((8, 3, 4, *block), F32),
            pltpu.VMEM((2, 4, 4, *block), F32),
            pltpu.VMEM((2, 3, 4, *block), F32),
            pltpu.VMEM((8, *block), F32),
            pltpu.VMEM((7, *block), F32),
            pltpu.VMEM(tall, F32),
            pltpu.VMEM((15, 32, LANES), F32),
            pltpu.VMEM(tall, F32),
            pltpu.VMEM((15, 32, LANES), F32),
            pltpu.VMEM((WIDTH // 2, SLICE), F32),
            pltpu.VMEM((WIDTH // 2, SLICE), F32),
            pltpu.VMEM((WIDTH // 2, SLICE), BF16),
            pltpu.VMEM((8, 16, LANES), F32),
            pltpu.VMEM((7, 16, LANES), F32),
            pltpu.VMEM(block, F32),
            pltpu.VMEM(block, F32),
            pltpu.VMEM(block, F32),
            pltpu.VMEM(block, F32),
            dma((PARTS + 5,)),
            dma((8,)),
            dma((8,)),
            dma((8,)),
            dma((2,)),
            dma((8,)),
            dma((11,)),
        ],
        compiler_params=pltpu.CompilerParams(
            collective_id=0, has_side_effects=True, vmem_limit_bytes=63 * 1024 * 1024
        ),
        name="distill",
    )(client_counts, sample_ids, logits, student_hidden, student_weight, perm)
    grad_weight, turned = pl.pallas_call(
        finish,
        out_shape=(
            jax.ShapeDtypeStruct((WIDTH, SLICE), BF16),
            jax.ShapeDtypeStruct((16, SAMPLES), F32),
        ),
        in_specs=[vmem] * 3,
        out_specs=(any_spec, vmem),
        scratch_shapes=[pltpu.VMEM((WIDTH, SLICE), BF16), dma((4,))],
        compiler_params=pltpu.CompilerParams(vmem_limit_bytes=8 * 1024 * 1024),
        name="finish",
    )(grad, grad_hidden, student_hidden)
    return grad_weight, turned.T


def solution(mesh):
    both = ("hst", "local")
    return jax.shard_map(
        per_device,
        mesh=mesh,
        in_specs=(P(both, None, None), P(both, None), P(both), P(), P(None, both)),
        out_specs=(P(None, both), P(None, both)),
        check_vma=False,
    )
```

```python
import jax
import jax.numpy as jnp
from jax import lax
from jax.experimental import pallas as pl
from jax.experimental.pallas import tpu as pltpu
from jax.sharding import PartitionSpec as P

MESH = pl.DeviceIdType.MESH
F32 = jnp.float32
BF16 = jnp.bfloat16
SAMPLES = 24
VOCAB = 32000
WIDTH = 4096
SLICE = 125
LANES = 128
SCALE = 32768.0 / SAMPLES
Z_FAR_FIRST = (4, 3, 5, 2, 6, 1, 7)
FAR_FIRST = (10, 6, 9, 11, 14, 2, 8, 5, 7, 13, 15, 1, 3, 4, 12)
STEP_COLUMNS = 512
STEPS = tuple(-(-min(4000 * (k + 1) + LANES, VOCAB) // STEP_COLUMNS) for k in range(8))
PARTS = 8
WINDOW = 17
LAG = 4
DIRECT = 1
ALONG_Z = 4 - DIRECT
LOW = -3.0e38


def remote(src, dst, send_sem, recv_sem, hst, loc):
    return pltpu.make_async_remote_copy(
        src_ref=src,
        dst_ref=dst,
        send_sem=send_sem,
        recv_sem=recv_sem,
        device_id={"hst": hst, "local": loc},
        device_id_type=MESH,
    )


def lane_index(rows):
    return lax.broadcasted_iota(jnp.int32, (rows, LANES), 1)


def masked_top(values):
    return jnp.max(
        jnp.where(lane_index(SAMPLES) < SLICE, values, LOW), axis=1, keepdims=True
    )


def weighted_product(values, top, rows):
    valid = lane_index(SAMPLES) < SLICE
    weights = jnp.where(valid, jnp.exp(values - top), 0.0)
    product = lax.dot_general(
        split_two(weights), rows, (((1,), (1,)), ((), ())), preferred_element_type=F32
    )
    return jnp.sum(weights, axis=1, keepdims=True), product[:SAMPLES] + product[SAMPLES:]


def packed_stats(top, total):
    lane = lane_index(8)
    tile = jnp.zeros((8, LANES), F32)
    for r in range(3):
        tile = jnp.where((lane >= 16 * r) & (lane < 16 * r + 16), top[8 * r : 8 * r + 8], tile)
        low = 48 + 16 * r
        tile = jnp.where((lane >= low) & (lane < low + 16), total[8 * r : 8 * r + 8], tile)
    return tile


def split_two(weights):
    high = weights.astype(BF16)
    low = (weights - high.astype(F32)).astype(BF16)
    return jnp.concatenate([high, low], axis=0)[:, :SLICE]


def own_part(own, rows, out):
    top = masked_top(own)
    total, product = weighted_product(own, top, rows)
    for b in range(16):
        out[b, 0:SAMPLES, :] = product[:, LANES * b : LANES * (b + 1)]
    return top, total


def other_part(top, total, other, rows, out):
    joined = jnp.maximum(top, masked_top(other))
    more, product = weighted_product(other, joined, rows)
    scale = jnp.exp(top - joined)
    stats = packed_stats(joined, total * scale + more)
    for b in range(16):
        out[b, 0:SAMPLES, :] = (
            out[b, 0:SAMPLES, :] * scale + product[:, LANES * b : LANES * (b + 1)]
        )
        out[b, SAMPLES:32, :] = stats


def factors(stat, joined):
    scale = jnp.exp(stat - joined)
    return scale, [scale[:, 16 * r : 16 * r + 1] for r in range(3)]


def join_plane(own, here, came):
    mine = own[here]
    stats = [mine[SAMPLES:32]] + [came[k, SAMPLES:32, :] for k in range(15)]
    joined = stats[0]
    for stat in stats[1:]:
        joined = jnp.maximum(joined, stat)
    total = jnp.zeros((8, LANES), F32)
    sums = [jnp.zeros((8, LANES), F32) for _ in range(3)]
    for k in range(16):
        scale, rows = factors(stats[k], joined)
        total = total + stats[k] * pltpu.roll(scale, 48, 1)
        for r in range(3):
            block = mine[8 * r : 8 * r + 8] if k == 0 else came[k - 1, 8 * r : 8 * r + 8, :]
            sums[r] = sums[r] + block * rows[r]
    tops = [joined[:, 16 * r : 16 * r + 1] for r in range(3)]
    totals = [total[:, 48 + 16 * r : 49 + 16 * r] for r in range(3)]
    return sums, tops, totals


def kernel(
    counts_hbm, ids_hbm, logits_hbm, hidden_hbm, weight_hbm, perm_hbm,
    grad_ref, hidden_out,
    counts, ids, x_in, local, hidden, weight, w_perm,
    count_to, count_from, blocks, from_core,
    got1, second, got2, third, from_z, c_from, c_sum, c_got,
    t_own, t_plane, s_own, s_plane, w_to, w_from, w_other,
    z_to, z_from, teacher, student, s_other, t_other,
    load_sems, core_recv, ring_recv, cross_recv, many_recv, send_sems,
):
    hst, loc = lax.axis_index("hst"), lax.axis_index("local")
    z, c = hst // 2, hst % 2
    y, x = loc // 4, loc % 4
    other = z * 2 + (1 - c)

    early = [
        pltpu.make_async_copy(ids_hbm, ids, load_sems.at[PARTS]),
        pltpu.make_async_copy(counts_hbm, counts, load_sems.at[PARTS + 1]),
    ]
    loads = [
        pltpu.make_async_copy(
            logits_hbm.at[:, pl.ds(low, high - low)], x_in.at[:, pl.ds(low, high - low)],
            load_sems.at[k],
        )
        for k, (low, high) in enumerate(
            (STEP_COLUMNS * ((0,) + STEPS)[k], min(STEP_COLUMNS * STEPS[k], VOCAB))
            for k in range(PARTS)
        )
    ]
    for load in early + loads[:1]:
        load.start()

    barrier = pltpu.get_barrier_semaphore()

    def greet(to_hst, to_loc):
        pl.semaphore_signal(
            barrier, inc=1, device_id={"hst": to_hst, "local": to_loc}, device_id_type=MESH
        )

    for k in range(1, 8):
        greet(((z + k) % 8) * 2 + c, loc)
    for k in FAR_FIRST:
        greet(hst, ((y + k // 4) % 4) * 4 + (x + k % 4) % 4)
    greet(other, loc)

    for load in loads[1:]:
        load.start()
    late = [
        pltpu.make_async_copy(hidden_hbm, hidden, load_sems.at[PARTS + 2]),
        pltpu.make_async_copy(weight_hbm, weight, load_sems.at[PARTS + 3]),
    ]
    for load in late:
        load.start()
    for a in range(8):
        for b in range(2):
            pltpu.make_async_copy(
                perm_hbm.at[a, b], w_perm.at[b, :, :, a], load_sems.at[PARTS + 4]
            ).start()
    late.append(pltpu.make_async_copy(w_perm, w_perm, load_sems.at[PARTS + 4]))
    for load in early:
        load.wait()

    place = lax.broadcasted_iota(jnp.int32, (SAMPLES, SAMPLES), 0)
    highs, lows = [], []
    for client in range(2):
        chosen = ids[client : client + 1, :] == place
        high = (counts[client] // 256) * 256
        highs.append(jnp.where(chosen, high.astype(F32), 0.0))
        lows.append(jnp.where(chosen, (counts[client] - high).astype(F32), 0.0))
    one = jnp.concatenate(highs + lows, axis=1)
    none = jnp.zeros_like(one)
    selector = jnp.concatenate(
        [jnp.concatenate([one, none], axis=1), jnp.concatenate([none, one], axis=1)], axis=0
    ).astype(BF16)
    count_sum = (counts[0] + counts[1]).astype(F32)
    count_to[...] = jnp.full((8, LANES), count_sum, F32)
    local[VOCAB // LANES] = jnp.zeros((SAMPLES, LANES), F32)
    lane = lane_index(SAMPLES)
    valid = lane < SLICE

    def multiply(step):
        at = step * STEP_COLUMNS
        groups = min(2, (VOCAB - at) // 256)
        columns = [x_in[:, at + 256 * g : at + 256 * (g + 1)] for g in range(groups)]
        stacked = jnp.concatenate([part for part in columns for _ in range(2)], axis=0)
        sums = jnp.dot(
            selector[: 24 * groups, : 96 * groups], stacked, preferred_element_type=F32
        )
        for g in range(groups):
            tile = at // LANES + 2 * g
            local[tile] = sums[24 * g : 24 * g + 24, :LANES]
            local[tile + 1] = sums[24 * g : 24 * g + 24, LANES:]

    places = []
    for color in range(2):
        for k in range(16):
            dx, dy = (k + 4 - x) % 4, (k // 4 + 4 - y) % 4
            along, across = (dy, dx) if color else (dx, dy)
            places.append(along * 4 + across)

    def first_tile(k, side):
        return (32 * k + 16 * side) * SLICE // LANES

    along_x = [y * 4 + (x + n) % 4 for n in range(4)]
    along_y = [((y + n) % 4) * 4 + x for n in range(4)]
    ways = (along_x, along_y)
    core_copies = []

    def send(src, dst, sem, recv_sem, to_hst, to_loc):
        copy = remote(src, dst, send_sems.at[sem], recv_sem, to_hst, to_loc)
        copy.start()
        return copy

    def arrived(ref, recv_sem):
        pltpu.make_async_copy(ref, ref, recv_sem).wait()

    def group(k, n, low=0, count=4):
        return blocks.at[pl.ds(16 * k + 4 * n + low, count)]

    def receive_core(k):
        core_copies[k].wait_recv()
        counted = count_from[0:1, :] + count_sum
        for side_c in range(2):

            @pl.when(c == side_c)
            def cut(side_c=side_c):
                base = first_tile(k, side_c)
                for n in range(16):
                    begin = (32 * k + 16 * side_c + n) * SLICE
                    tile, shift = begin // LANES, begin % LANES
                    block = local[tile] + from_core[k, tile - base]
                    if shift + SLICE > LANES:
                        after = local[tile + 1] + from_core[k, tile + 1 - base]
                        block = jnp.where(lane >= shift, block, after)
                    if shift:
                        block = pltpu.roll(block, LANES - shift, 1)
                    blocks[16 * k + places[16 * (k % 2) + n]] = jnp.where(valid, block, counted)


        @pl.when(z != k)
        def along_z():
            came_from = (k + 8 - z) % 8
            send(
                group(k, 2, DIRECT, ALONG_Z), c_from.at[came_from - 1], 11, many_recv.at[8],
                2 * k + c, loc,
            )

        way = ways[k % 2]
        if DIRECT:
            send(
                group(k, 2, 0, DIRECT), got1.at[k, pl.ds(8, DIRECT)], 1, ring_recv.at[k],
                hst, way[2],
            )
        send(group(k, 1), got1.at[k, pl.ds(0, 4)], 1, ring_recv.at[k], hst, way[1])
        send(group(k, 3), got1.at[k, pl.ds(4, 4)], 1, ring_recv.at[k], hst, way[3])

    for k in range(8):
        loads[k].wait()
        for step in range(((0,) + STEPS)[k], STEPS[k]):
            multiply(step)
        if k == 0:
            pl.semaphore_wait(barrier, 23)
            count_copy = send(count_to, count_from, 9, many_recv.at[6], other, loc)
        window = c * first_tile(k, 0) + (1 - c) * first_tile(k, 1)
        core_copies.append(
            send(
                local.at[pl.ds(window, WINDOW)], from_core.at[k], 0, core_recv.at[k], other, loc
            )
        )
        if k >= LAG:
            if k == LAG:
                count_copy.wait_recv()
            receive_core(k - LAG)
    for k in range(8 - LAG, 8):
        receive_core(k)
    for load in late:
        load.wait()

    @pl.when(c == 0)
    def widen_second():
        w_to[...] = w_perm[1].reshape(WIDTH // 2, SLICE).astype(F32)

    @pl.when(c == 1)
    def widen_first():
        w_to[...] = w_perm[0].reshape(WIDTH // 2, SLICE).astype(F32)

    w_copy = send(w_to, w_from, 5, many_recv.at[0], other, loc)
    student[:, :SLICE] = jnp.dot(hidden[...], weight[...], preferred_element_type=F32)
    student[:, SLICE:] = jnp.zeros((SAMPLES, LANES - SLICE), F32)
    s_copy = send(student, s_other, 7, many_recv.at[1], other, loc)
    w_copy.wait_recv()
    w_other[...] = w_from[...].astype(BF16)
    s_copy.wait_recv()
    own_rows = w_perm[c].reshape(WIDTH // 2, SLICE)
    top, total = own_part(student[...], own_rows, s_own)
    other_part(top, total, s_other[...], w_other[...], s_own)

    for half in range(2):
        for k in range(4 * half, 4 * half + 4):
            arrived(got1.at[k], ring_recv.at[k])
            for n in range(4):
                total = blocks[16 * k + n] + (got1[k, n] + got1[k, 4 + n])
                if n < DIRECT:
                    total = total + got1[k, 8 + n]
                second[half, k % 2, n, k // 2 - 2 * half] = total
        for n in (2, 1, 3):
            for color in range(2):
                send(
                    second.at[half, color, n], got2.at[half, color, n - 1], 2,
                    cross_recv.at[half], hst, ways[1 - color][n],
                )
    arrived(c_from, many_recv.at[8])
    odd = z % 2
    for n in range(ALONG_Z):
        at = 16 * z + 8 + DIRECT + n
        total = blocks[at]
        for k in range(7):
            total = total + c_from[k, n]
        c_sum[n] = total
        across = DIRECT + n
        to_x = (x + 2 * (1 - odd) + across * odd) % 4
        to_y = (y + 2 * odd + across * (1 - odd)) % 4
        send(c_sum.at[n], c_got.at[n], 12, many_recv.at[9], hst, to_y * 4 + to_x)
    for half in range(2):
        arrived(got2.at[half], cross_recv.at[half])
        for item in range(2):
            for color in range(2):
                to_z = 4 * half + 2 * item + color
                third[to_z] = (second[half, color, 0, item] + got2[half, color, 0, item]) + (
                    got2[half, color, 1, item] + got2[half, color, 2, item]
                )
        for to_z in range(4 * half, 4 * half + 4):

            @pl.when(z != to_z)
            def to_owner(to_z=to_z):
                slot = (to_z + 8 - z) % 8 - 1
                send(third.at[to_z], from_z.at[slot], 3, many_recv.at[2], 2 * to_z + c, loc)

    def plane(src, dst, sem, recv_sem):
        for k in FAR_FIRST:
            to = ((y + k // 4) % 4) * 4 + (x + k % 4) % 4
            send(src.at[to], dst.at[k - 1], sem, recv_sem, hst, to)

    plane(s_own, s_plane, 6, many_recv.at[3])
    arrived(from_z, many_recv.at[2])
    summed = third[z]
    for k in range(7):
        summed = summed + from_z[k]
    arrived(c_got, many_recv.at[9])
    for n in range(ALONG_Z):
        summed = summed + c_got[n]

    ensemble = summed / summed[:, SLICE : SLICE + 1]
    teacher[...] = ensemble
    t_copy = send(teacher, t_other, 10, many_recv.at[7], other, loc)
    top, total = own_part(ensemble, own_rows, t_own)
    t_copy.wait_recv()
    other_part(top, total, t_other[...], w_other[...], t_own)
    plane(t_own, t_plane, 8, many_recv.at[4])

    arrived(s_plane, many_recv.at[3])
    s_sums, s_tops, s_totals = join_plane(s_own, loc, s_plane)
    lane8 = lane_index(8)

    def spread(sums, tops, totals, base, tile, tops_tile):
        for r in range(3):
            low = base + 20 * r
            inside = (lane8 >= low) & (lane8 < low + 16)
            ending = (lane8 >= low + 16) & (lane8 < low + 20)
            for k in range(8):
                moved = pltpu.roll(sums[r], (low - 16 * k) % LANES, 1)
                tile[k] = jnp.where(ending, totals[r], jnp.where(inside, moved, tile[k]))
            tops_tile = jnp.where(inside | ending, tops[r], tops_tile)
        return tops_tile

    tiles = [jnp.zeros((8, LANES), F32) for _ in range(8)]
    tops_tile = spread(s_sums, s_tops, s_totals, 60, tiles, jnp.zeros((8, LANES), F32))
    arrived(t_plane, many_recv.at[4])
    t_sums, t_tops, t_totals = join_plane(t_own, loc, t_plane)
    tops_tile = spread(t_sums, t_tops, t_totals, 0, tiles, tops_tile)
    for k in range(8):
        z_to[k, 0:8, :] = tiles[k]
        z_to[k, 8:16, :] = tops_tile
    for k in Z_FAR_FIRST:
        to_z = (z + k) % 8
        send(z_to.at[to_z], z_from.at[k - 1], 4, many_recv.at[5], to_z * 2 + c, loc)
    arrived(z_from, many_recv.at[5])
    mine = z_to[z]
    pieces = [mine] + [z_from[k] for k in range(7)]
    joined = pieces[0][8:16]
    for piece in pieces[1:]:
        joined = jnp.maximum(joined, piece[8:16])
    sums = jnp.zeros((8, LANES), F32)
    for piece in pieces:
        sums = sums + piece[0:8] * jnp.exp(piece[8:16] - joined)

    for r in range(3):
        t_low, s_low = 20 * r, 60 + 20 * r
        t_top, s_top = joined[:, t_low : t_low + 1], joined[:, s_low : s_low + 1]
        t_total = sums[:, t_low + 16 : t_low + 17]
        s_total = sums[:, s_low + 16 : s_low + 17]
        rows = slice(8 * r, 8 * r + 8)
        t_part = pltpu.roll(sums, (LANES - t_low) % LANES, 1) / t_total
        s_part = pltpu.roll(sums, (LANES - s_low) % LANES, 1) / s_total
        hidden_out[rows, :] = (SCALE * (s_part - t_part))[:, :16]
        s_prob = jnp.exp(student[rows, :] - s_top) / s_total
        t_prob = jnp.exp(teacher[rows, :] - t_top) / t_total
        grad_ref[rows, :] = (SCALE * (s_prob - t_prob))[:, :SLICE]

    for n, ref in enumerate(
        (from_core, got1, got2, from_z, z_from, w_to, s_plane, student, t_plane, count_to, teacher, c_from, c_got)
    ):
        arrived(ref, send_sems.at[n])


def finish(grad, grad_hidden, hidden, weight_out, hidden_out, rows, sems):
    rounded = grad[...].astype(BF16)
    size = WIDTH // 4
    copies = []
    for k in range(4):
        part = pl.ds(k * size, size)
        rows[part, :] = lax.dot_general(
            hidden[:, part], rounded, (((0,), (0,)), ((), ())), preferred_element_type=F32
        ).astype(BF16)
        copies.append(pltpu.make_async_copy(rows.at[part], weight_out.at[part], sems.at[k]))
        copies[k].start()
    hidden_out[...] = grad_hidden[...].T
    for copy in copies:
        copy.wait()


def per_device(teacher_logits, sample_ids, client_counts, student_hidden, student_weight):
    logits = teacher_logits.reshape(2 * SAMPLES, VOCAB)
    perm = student_weight.reshape(8, 2, 4, 4, 16, SLICE)
    any_spec = pl.BlockSpec(memory_space=pltpu.HBM)
    vmem = pl.BlockSpec(memory_space=pltpu.VMEM)
    block = (SAMPLES, LANES)
    tall = (16, 32, LANES)
    dma = pltpu.SemaphoreType.DMA
    grad, grad_hidden = pl.pallas_call(
        kernel,
        out_shape=(
            pltpu.VMEM((SAMPLES, SLICE), F32),
            pltpu.VMEM((SAMPLES, 16), F32),
        ),
        in_specs=[any_spec] * 6,
        out_specs=(vmem, vmem),
        scratch_shapes=[
            pltpu.SMEM((2,), jnp.int32),
            pltpu.VMEM((2, SAMPLES), jnp.int32),
            pltpu.VMEM((2 * SAMPLES, VOCAB), BF16),
            pltpu.VMEM((VOCAB // LANES + 2, *block), F32),
            pltpu.VMEM((SAMPLES, WIDTH), BF16),
            pltpu.VMEM((WIDTH, SLICE), BF16),
            pltpu.VMEM((2, 4, 4, 8, 16, SLICE), BF16),
            pltpu.VMEM((8, LANES), F32),
            pltpu.VMEM((8, LANES), F32),
            pltpu.VMEM((128, *block), F32),
            pltpu.VMEM((8, WINDOW, *block), F32),
            pltpu.VMEM((8, 8 + DIRECT, *block), F32),
            pltpu.VMEM((2, 2, 4, 2, *block), F32),
            pltpu.VMEM((2, 2, 3, 2, *block), F32),
            pltpu.VMEM((8, *block), F32),
            pltpu.VMEM((7, *block), F32),
            pltpu.VMEM((7, ALONG_Z, *block), F32),
            pltpu.VMEM((ALONG_Z, *block), F32),
            pltpu.VMEM((ALONG_Z, *block), F32),
            pltpu.VMEM(tall, F32),
            pltpu.VMEM((15, 32, LANES), F32),
            pltpu.VMEM(tall, F32),
            pltpu.VMEM((15, 32, LANES), F32),
            pltpu.VMEM((WIDTH // 2, SLICE), F32),
            pltpu.VMEM((WIDTH // 2, SLICE), F32),
            pltpu.VMEM((WIDTH // 2, SLICE), BF16),
            pltpu.VMEM((8, 16, LANES), F32),
            pltpu.VMEM((7, 16, LANES), F32),
            pltpu.VMEM(block, F32),
            pltpu.VMEM(block, F32),
            pltpu.VMEM(block, F32),
            pltpu.VMEM(block, F32),
            dma((PARTS + 5,)),
            dma((8,)),
            dma((8,)),
            dma((2,)),
            dma((10,)),
            dma((13,)),
        ],
        compiler_params=pltpu.CompilerParams(
            collective_id=0, has_side_effects=True, vmem_limit_bytes=63 * 1024 * 1024
        ),
        name="distill",
    )(client_counts, sample_ids, logits, student_hidden, student_weight, perm)
    grad_weight, turned = pl.pallas_call(
        finish,
        out_shape=(
            jax.ShapeDtypeStruct((WIDTH, SLICE), BF16),
            jax.ShapeDtypeStruct((16, SAMPLES), F32),
        ),
        in_specs=[vmem] * 3,
        out_specs=(any_spec, vmem),
        scratch_shapes=[pltpu.VMEM((WIDTH, SLICE), BF16), dma((4,))],
        compiler_params=pltpu.CompilerParams(vmem_limit_bytes=8 * 1024 * 1024),
        name="finish",
    )(grad, grad_hidden, student_hidden)
    return grad_weight, turned.T


def solution(mesh):
    both = ("hst", "local")
    return jax.shard_map(
        per_device,
        mesh=mesh,
        in_specs=(P(both, None, None), P(both, None), P(both), P(), P(None, both)),
        out_specs=(P(None, both), P(None, both)),
        check_vma=False,
    )
```

```python
import jax
import jax.numpy as jnp
from jax import lax
from jax.experimental import pallas as pl
from jax.experimental.pallas import tpu as pltpu
from jax.sharding import PartitionSpec as P

MESH = pl.DeviceIdType.MESH
F32 = jnp.float32
BF16 = jnp.bfloat16
SAMPLES = 24
VOCAB = 32000
WIDTH = 4096
SLICE = 125
LANES = 128
SCALE = 32768.0 / SAMPLES
Z_FAR_FIRST = (4, 3, 5, 2, 6, 1, 7)
FAR_FIRST = (10, 6, 9, 11, 14, 2, 8, 5, 7, 13, 15, 1, 3, 4, 12)
STEP_COLUMNS = 512
STEPS = tuple(-(-min(4000 * (k + 1) + LANES, VOCAB) // STEP_COLUMNS) for k in range(8))
PARTS = 8
WINDOW = 17
LAG = 4
ITEMS = ((0, 2), (2, 1), (3, 1))
DIRECT = 1
ALONG_Z = 4 - DIRECT
LOW = -3.0e38


def remote(src, dst, send_sem, recv_sem, hst, loc):
    return pltpu.make_async_remote_copy(
        src_ref=src,
        dst_ref=dst,
        send_sem=send_sem,
        recv_sem=recv_sem,
        device_id={"hst": hst, "local": loc},
        device_id_type=MESH,
    )


def lane_index(rows):
    return lax.broadcasted_iota(jnp.int32, (rows, LANES), 1)


def masked_top(values):
    return jnp.max(
        jnp.where(lane_index(SAMPLES) < SLICE, values, LOW), axis=1, keepdims=True
    )


def weighted_product(values, top, rows):
    valid = lane_index(SAMPLES) < SLICE
    weights = jnp.where(valid, jnp.exp(values - top), 0.0)
    product = lax.dot_general(
        split_two(weights), rows, (((1,), (1,)), ((), ())), preferred_element_type=F32
    )
    return jnp.sum(weights, axis=1, keepdims=True), product[:SAMPLES] + product[SAMPLES:]


def packed_stats(top, total):
    lane = lane_index(8)
    tile = jnp.zeros((8, LANES), F32)
    for r in range(3):
        tile = jnp.where((lane >= 16 * r) & (lane < 16 * r + 16), top[8 * r : 8 * r + 8], tile)
        low = 48 + 16 * r
        tile = jnp.where((lane >= low) & (lane < low + 16), total[8 * r : 8 * r + 8], tile)
    return tile


def split_two(weights):
    high = weights.astype(BF16)
    low = (weights - high.astype(F32)).astype(BF16)
    return jnp.concatenate([high, low], axis=0)[:, :SLICE]


def own_part(own, rows, out):
    top = masked_top(own)
    total, product = weighted_product(own, top, rows)
    for b in range(16):
        out[b, 0:SAMPLES, :] = product[:, LANES * b : LANES * (b + 1)]
    return top, total


def other_part(top, total, other, rows, out):
    joined = jnp.maximum(top, masked_top(other))
    more, product = weighted_product(other, joined, rows)
    scale = jnp.exp(top - joined)
    stats = packed_stats(joined, total * scale + more)
    for b in range(16):
        out[b, 0:SAMPLES, :] = (
            out[b, 0:SAMPLES, :] * scale + product[:, LANES * b : LANES * (b + 1)]
        )
        out[b, SAMPLES:32, :] = stats


def factors(stat, joined):
    scale = jnp.exp(stat - joined)
    return scale, [scale[:, 16 * r : 16 * r + 1] for r in range(3)]


def join_plane(own, here, came):
    mine = own[here]
    stats = [mine[SAMPLES:32]] + [came[k, SAMPLES:32, :] for k in range(15)]
    joined = stats[0]
    for stat in stats[1:]:
        joined = jnp.maximum(joined, stat)
    total = jnp.zeros((8, LANES), F32)
    sums = [jnp.zeros((8, LANES), F32) for _ in range(3)]
    for k in range(16):
        scale, rows = factors(stats[k], joined)
        total = total + stats[k] * pltpu.roll(scale, 48, 1)
        for r in range(3):
            block = mine[8 * r : 8 * r + 8] if k == 0 else came[k - 1, 8 * r : 8 * r + 8, :]
            sums[r] = sums[r] + block * rows[r]
    tops = [joined[:, 16 * r : 16 * r + 1] for r in range(3)]
    totals = [total[:, 48 + 16 * r : 49 + 16 * r] for r in range(3)]
    return sums, tops, totals


def kernel(
    counts_hbm, ids_hbm, logits_hbm, hidden_hbm, weight_hbm, perm_hbm,
    grad_ref, hidden_out,
    counts, ids, x_in, local, hidden, weight, w_perm,
    count_to, count_from, blocks, from_core,
    got1, second, got2, third, from_z, c_from, c_sum, c_got,
    t_own, t_plane, s_own, s_plane, w_to, w_from, w_other,
    z_to, z_from, teacher, student, s_other, t_other,
    load_sems, core_recv, ring_recv, cross_recv, many_recv, send_sems,
):
    hst, loc = lax.axis_index("hst"), lax.axis_index("local")
    z, c = hst // 2, hst % 2
    y, x = loc // 4, loc % 4
    other = z * 2 + (1 - c)

    early = [
        pltpu.make_async_copy(ids_hbm, ids, load_sems.at[PARTS]),
        pltpu.make_async_copy(counts_hbm, counts, load_sems.at[PARTS + 1]),
    ]
    loads = [
        pltpu.make_async_copy(
            logits_hbm.at[:, pl.ds(low, high - low)], x_in.at[:, pl.ds(low, high - low)],
            load_sems.at[k],
        )
        for k, (low, high) in enumerate(
            (STEP_COLUMNS * ((0,) + STEPS)[k], min(STEP_COLUMNS * STEPS[k], VOCAB))
            for k in range(PARTS)
        )
    ]
    for load in early + loads[:1]:
        load.start()

    barrier = pltpu.get_barrier_semaphore()

    def greet(to_hst, to_loc):
        pl.semaphore_signal(
            barrier, inc=1, device_id={"hst": to_hst, "local": to_loc}, device_id_type=MESH
        )

    for k in range(1, 8):
        greet(((z + k) % 8) * 2 + c, loc)
    for k in FAR_FIRST:
        greet(hst, ((y + k // 4) % 4) * 4 + (x + k % 4) % 4)
    greet(other, loc)

    for load in loads[1:]:
        load.start()
    late = [
        pltpu.make_async_copy(hidden_hbm, hidden, load_sems.at[PARTS + 2]),
        pltpu.make_async_copy(weight_hbm, weight, load_sems.at[PARTS + 3]),
    ]
    for load in late:
        load.start()
    for a in range(8):
        for b in range(2):
            pltpu.make_async_copy(
                perm_hbm.at[a, b], w_perm.at[b, :, :, a], load_sems.at[PARTS + 4]
            ).start()
    late.append(pltpu.make_async_copy(w_perm, w_perm, load_sems.at[PARTS + 4]))
    for load in early:
        load.wait()

    place = lax.broadcasted_iota(jnp.int32, (SAMPLES, SAMPLES), 0)
    highs, lows = [], []
    for client in range(2):
        chosen = ids[client : client + 1, :] == place
        high = (counts[client] // 256) * 256
        highs.append(jnp.where(chosen, high.astype(F32), 0.0))
        lows.append(jnp.where(chosen, (counts[client] - high).astype(F32), 0.0))
    one = jnp.concatenate(highs + lows, axis=1)
    none = jnp.zeros_like(one)
    selector = jnp.concatenate(
        [jnp.concatenate([one, none], axis=1), jnp.concatenate([none, one], axis=1)], axis=0
    ).astype(BF16)
    count_sum = (counts[0] + counts[1]).astype(F32)
    count_to[...] = jnp.full((8, LANES), count_sum, F32)
    local[VOCAB // LANES] = jnp.zeros((SAMPLES, LANES), F32)
    lane = lane_index(SAMPLES)
    valid = lane < SLICE

    def multiply(step):
        at = step * STEP_COLUMNS
        groups = min(2, (VOCAB - at) // 256)
        columns = [x_in[:, at + 256 * g : at + 256 * (g + 1)] for g in range(groups)]
        stacked = jnp.concatenate([part for part in columns for _ in range(2)], axis=0)
        sums = jnp.dot(
            selector[: 24 * groups, : 96 * groups], stacked, preferred_element_type=F32
        )
        for g in range(groups):
            tile = at // LANES + 2 * g
            local[tile] = sums[24 * g : 24 * g + 24, :LANES]
            local[tile + 1] = sums[24 * g : 24 * g + 24, LANES:]

    places = []
    for color in range(2):
        for k in range(16):
            dx, dy = (k + 4 - x) % 4, (k // 4 + 4 - y) % 4
            along, across = (dy, dx) if color else (dx, dy)
            places.append(along * 4 + across)

    def first_tile(k, side):
        return (32 * k + 16 * side) * SLICE // LANES

    along_x = [y * 4 + (x + n) % 4 for n in range(4)]
    along_y = [((y + n) % 4) * 4 + x for n in range(4)]
    ways = (along_x, along_y)
    core_copies = []

    def send(src, dst, sem, recv_sem, to_hst, to_loc):
        copy = remote(src, dst, send_sems.at[sem], recv_sem, to_hst, to_loc)
        copy.start()
        return copy

    def arrived(ref, recv_sem):
        pltpu.make_async_copy(ref, ref, recv_sem).wait()

    def group(k, n, low=0, count=4):
        return blocks.at[pl.ds(16 * k + 4 * n + low, count)]

    def receive_core(k):
        core_copies[k].wait_recv()
        counted = count_from[0:1, :] + count_sum
        for side_c in range(2):

            @pl.when(c == side_c)
            def cut(side_c=side_c):
                base = first_tile(k, side_c)
                for n in range(16):
                    begin = (32 * k + 16 * side_c + n) * SLICE
                    tile, shift = begin // LANES, begin % LANES
                    block = local[tile] + from_core[k, tile - base]
                    if shift + SLICE > LANES:
                        after = local[tile + 1] + from_core[k, tile + 1 - base]
                        block = jnp.where(lane >= shift, block, after)
                    if shift:
                        block = pltpu.roll(block, LANES - shift, 1)
                    blocks[16 * k + places[16 * (k % 2) + n]] = jnp.where(valid, block, counted)


        @pl.when(z != k)
        def along_z():
            came_from = (k + 8 - z) % 8
            send(
                group(k, 2, DIRECT, ALONG_Z), c_from.at[came_from - 1], 11, many_recv.at[8],
                2 * k + c, loc,
            )

        way = ways[k % 2]
        if DIRECT:
            send(
                group(k, 2, 0, DIRECT), got1.at[k, pl.ds(8, DIRECT)], 1, ring_recv.at[k],
                hst, way[2],
            )
        send(group(k, 1), got1.at[k, pl.ds(0, 4)], 1, ring_recv.at[k], hst, way[1])
        send(group(k, 3), got1.at[k, pl.ds(4, 4)], 1, ring_recv.at[k], hst, way[3])

    for k in range(8):
        loads[k].wait()
        for step in range(((0,) + STEPS)[k], STEPS[k]):
            multiply(step)
        if k == 0:
            pl.semaphore_wait(barrier, 23)
            count_copy = send(count_to, count_from, 9, many_recv.at[6], other, loc)
        window = c * first_tile(k, 0) + (1 - c) * first_tile(k, 1)
        core_copies.append(
            send(
                local.at[pl.ds(window, WINDOW)], from_core.at[k], 0, core_recv.at[k], other, loc
            )
        )
        if k >= LAG:
            if k == LAG:
                count_copy.wait_recv()
            receive_core(k - LAG)
    for k in range(8 - LAG, 8):
        receive_core(k)
    for load in late:
        load.wait()

    @pl.when(c == 0)
    def widen_second():
        w_to[...] = w_perm[1].reshape(WIDTH // 2, SLICE).astype(F32)

    @pl.when(c == 1)
    def widen_first():
        w_to[...] = w_perm[0].reshape(WIDTH // 2, SLICE).astype(F32)

    w_copy = send(w_to, w_from, 5, many_recv.at[0], other, loc)
    student[:, :SLICE] = jnp.dot(hidden[...], weight[...], preferred_element_type=F32)
    student[:, SLICE:] = jnp.zeros((SAMPLES, LANES - SLICE), F32)
    s_copy = send(student, s_other, 7, many_recv.at[1], other, loc)
    w_copy.wait_recv()
    w_other[...] = w_from[...].astype(BF16)
    s_copy.wait_recv()
    own_rows = w_perm[c].reshape(WIDTH // 2, SLICE)
    top, total = own_part(student[...], own_rows, s_own)
    other_part(top, total, s_other[...], w_other[...], s_own)

    for part, (first_item, items) in enumerate(ITEMS):
        for k in range(2 * first_item, 2 * (first_item + items)):
            arrived(got1.at[k], ring_recv.at[k])
            for n in range(4):
                total = blocks[16 * k + n] + (got1[k, n] + got1[k, 4 + n])
                if n < DIRECT:
                    total = total + got1[k, 8 + n]
                second[k % 2, n, k // 2] = total
        taken = pl.ds(first_item, items)
        for n in (2, 1, 3):
            for color in range(2):
                send(
                    second.at[color, n, taken], got2.at[color, n - 1, taken], 2,
                    cross_recv.at[part], hst, ways[1 - color][n],
                )
    arrived(c_from, many_recv.at[8])
    odd = z % 2
    for n in range(ALONG_Z):
        at = 16 * z + 8 + DIRECT + n
        total = blocks[at]
        for k in range(7):
            total = total + c_from[k, n]
        c_sum[n] = total
        across = DIRECT + n
        to_x = (x + 2 * (1 - odd) + across * odd) % 4
        to_y = (y + 2 * odd + across * (1 - odd)) % 4
        send(c_sum.at[n], c_got.at[n], 12, many_recv.at[9], hst, to_y * 4 + to_x)
    for part, (first_item, items) in enumerate(ITEMS):
        arrived(got2.at[:, :, pl.ds(first_item, items)], cross_recv.at[part])
        for item in range(first_item, first_item + items):
            for color in range(2):
                third[2 * item + color] = (second[color, 0, item] + got2[color, 0, item]) + (
                    got2[color, 1, item] + got2[color, 2, item]
                )
        for n in range(2 * items):
            to_z = 2 * first_item + (z + 1 + n) % (2 * items)

            @pl.when(z != to_z)
            def to_owner(to_z=to_z):
                slot = (to_z + 8 - z) % 8 - 1
                send(third.at[to_z], from_z.at[slot], 3, many_recv.at[2], 2 * to_z + c, loc)

    def plane(src, dst, sem, recv_sem):
        for k in FAR_FIRST:
            to = ((y + k // 4) % 4) * 4 + (x + k % 4) % 4
            send(src.at[to], dst.at[k - 1], sem, recv_sem, hst, to)

    plane(s_own, s_plane, 6, many_recv.at[3])
    arrived(from_z, many_recv.at[2])
    summed = third[z]
    for k in range(7):
        summed = summed + from_z[k]
    arrived(c_got, many_recv.at[9])
    for n in range(ALONG_Z):
        summed = summed + c_got[n]

    ensemble = summed / summed[:, SLICE : SLICE + 1]
    teacher[...] = ensemble
    t_copy = send(teacher, t_other, 10, many_recv.at[7], other, loc)
    top, total = own_part(ensemble, own_rows, t_own)
    t_copy.wait_recv()
    other_part(top, total, t_other[...], w_other[...], t_own)
    plane(t_own, t_plane, 8, many_recv.at[4])

    arrived(s_plane, many_recv.at[3])
    s_sums, s_tops, s_totals = join_plane(s_own, loc, s_plane)
    lane8 = lane_index(8)

    def spread(sums, tops, totals, base, tile, tops_tile):
        for r in range(3):
            low = base + 20 * r
            inside = (lane8 >= low) & (lane8 < low + 16)
            ending = (lane8 >= low + 16) & (lane8 < low + 20)
            for k in range(8):
                moved = pltpu.roll(sums[r], (low - 16 * k) % LANES, 1)
                tile[k] = jnp.where(ending, totals[r], jnp.where(inside, moved, tile[k]))
            tops_tile = jnp.where(inside | ending, tops[r], tops_tile)
        return tops_tile

    tiles = [jnp.zeros((8, LANES), F32) for _ in range(8)]
    tops_tile = spread(s_sums, s_tops, s_totals, 60, tiles, jnp.zeros((8, LANES), F32))
    arrived(t_plane, many_recv.at[4])
    t_sums, t_tops, t_totals = join_plane(t_own, loc, t_plane)
    tops_tile = spread(t_sums, t_tops, t_totals, 0, tiles, tops_tile)
    for k in range(8):
        z_to[k, 0:8, :] = tiles[k]
        z_to[k, 8:16, :] = tops_tile
    for k in Z_FAR_FIRST:
        to_z = (z + k) % 8
        send(z_to.at[to_z], z_from.at[k - 1], 4, many_recv.at[5], to_z * 2 + c, loc)
    arrived(z_from, many_recv.at[5])
    mine = z_to[z]
    pieces = [mine] + [z_from[k] for k in range(7)]
    joined = pieces[0][8:16]
    for piece in pieces[1:]:
        joined = jnp.maximum(joined, piece[8:16])
    sums = jnp.zeros((8, LANES), F32)
    for piece in pieces:
        sums = sums + piece[0:8] * jnp.exp(piece[8:16] - joined)

    for r in range(3):
        t_low, s_low = 20 * r, 60 + 20 * r
        t_top, s_top = joined[:, t_low : t_low + 1], joined[:, s_low : s_low + 1]
        t_total = sums[:, t_low + 16 : t_low + 17]
        s_total = sums[:, s_low + 16 : s_low + 17]
        rows = slice(8 * r, 8 * r + 8)
        t_part = pltpu.roll(sums, (LANES - t_low) % LANES, 1) / t_total
        s_part = pltpu.roll(sums, (LANES - s_low) % LANES, 1) / s_total
        hidden_out[rows, :] = (SCALE * (s_part - t_part))[:, :16]
        s_prob = jnp.exp(student[rows, :] - s_top) / s_total
        t_prob = jnp.exp(teacher[rows, :] - t_top) / t_total
        grad_ref[rows, :] = (SCALE * (s_prob - t_prob))[:, :SLICE]

    for n, ref in enumerate(
        (from_core, got1, got2, from_z, z_from, w_to, s_plane, student, t_plane, count_to, teacher, c_from, c_got)
    ):
        arrived(ref, send_sems.at[n])


def finish(grad, grad_hidden, hidden, weight_out, hidden_out, rows, sems):
    rounded = grad[...].astype(BF16)
    size = WIDTH // 4
    copies = []
    for k in range(4):
        part = pl.ds(k * size, size)
        rows[part, :] = lax.dot_general(
            hidden[:, part], rounded, (((0,), (0,)), ((), ())), preferred_element_type=F32
        ).astype(BF16)
        copies.append(pltpu.make_async_copy(rows.at[part], weight_out.at[part], sems.at[k]))
        copies[k].start()
    hidden_out[...] = grad_hidden[...].T
    for copy in copies:
        copy.wait()


def per_device(teacher_logits, sample_ids, client_counts, student_hidden, student_weight):
    logits = teacher_logits.reshape(2 * SAMPLES, VOCAB)
    perm = student_weight.reshape(8, 2, 4, 4, 16, SLICE)
    any_spec = pl.BlockSpec(memory_space=pltpu.HBM)
    vmem = pl.BlockSpec(memory_space=pltpu.VMEM)
    block = (SAMPLES, LANES)
    tall = (16, 32, LANES)
    dma = pltpu.SemaphoreType.DMA
    grad, grad_hidden = pl.pallas_call(
        kernel,
        out_shape=(
            pltpu.VMEM((SAMPLES, SLICE), F32),
            pltpu.VMEM((SAMPLES, 16), F32),
        ),
        in_specs=[any_spec] * 6,
        out_specs=(vmem, vmem),
        scratch_shapes=[
            pltpu.SMEM((2,), jnp.int32),
            pltpu.VMEM((2, SAMPLES), jnp.int32),
            pltpu.VMEM((2 * SAMPLES, VOCAB), BF16),
            pltpu.VMEM((VOCAB // LANES + 2, *block), F32),
            pltpu.VMEM((SAMPLES, WIDTH), BF16),
            pltpu.VMEM((WIDTH, SLICE), BF16),
            pltpu.VMEM((2, 4, 4, 8, 16, SLICE), BF16),
            pltpu.VMEM((8, LANES), F32),
            pltpu.VMEM((8, LANES), F32),
            pltpu.VMEM((128, *block), F32),
            pltpu.VMEM((8, WINDOW, *block), F32),
            pltpu.VMEM((8, 8 + DIRECT, *block), F32),
            pltpu.VMEM((2, 4, 4, *block), F32),
            pltpu.VMEM((2, 3, 4, *block), F32),
            pltpu.VMEM((8, *block), F32),
            pltpu.VMEM((7, *block), F32),
            pltpu.VMEM((7, ALONG_Z, *block), F32),
            pltpu.VMEM((ALONG_Z, *block), F32),
            pltpu.VMEM((ALONG_Z, *block), F32),
            pltpu.VMEM(tall, F32),
            pltpu.VMEM((15, 32, LANES), F32),
            pltpu.VMEM(tall, F32),
            pltpu.VMEM((15, 32, LANES), F32),
            pltpu.VMEM((WIDTH // 2, SLICE), F32),
            pltpu.VMEM((WIDTH // 2, SLICE), F32),
            pltpu.VMEM((WIDTH // 2, SLICE), BF16),
            pltpu.VMEM((8, 16, LANES), F32),
            pltpu.VMEM((7, 16, LANES), F32),
            pltpu.VMEM(block, F32),
            pltpu.VMEM(block, F32),
            pltpu.VMEM(block, F32),
            pltpu.VMEM(block, F32),
            dma((PARTS + 5,)),
            dma((8,)),
            dma((8,)),
            dma((3,)),
            dma((10,)),
            dma((13,)),
        ],
        compiler_params=pltpu.CompilerParams(
            collective_id=0, has_side_effects=True, vmem_limit_bytes=63 * 1024 * 1024
        ),
        name="distill",
    )(client_counts, sample_ids, logits, student_hidden, student_weight, perm)
    grad_weight, turned = pl.pallas_call(
        finish,
        out_shape=(
            jax.ShapeDtypeStruct((WIDTH, SLICE), BF16),
            jax.ShapeDtypeStruct((16, SAMPLES), F32),
        ),
        in_specs=[vmem] * 3,
        out_specs=(any_spec, vmem),
        scratch_shapes=[pltpu.VMEM((WIDTH, SLICE), BF16), dma((4,))],
        compiler_params=pltpu.CompilerParams(vmem_limit_bytes=8 * 1024 * 1024),
        name="finish",
    )(grad, grad_hidden, student_hidden)
    return grad_weight, turned.T


def solution(mesh):
    both = ("hst", "local")
    return jax.shard_map(
        per_device,
        mesh=mesh,
        in_specs=(P(both, None, None), P(both, None), P(both), P(), P(None, both)),
        out_specs=(P(None, both), P(None, both)),
        check_vma=False,
    )
```

```python
import jax
import jax.numpy as jnp
from jax import lax
from jax.experimental import pallas as pl
from jax.experimental.pallas import tpu as pltpu
from jax.sharding import PartitionSpec as P

MESH = pl.DeviceIdType.MESH
F32 = jnp.float32
BF16 = jnp.bfloat16
SAMPLES = 24
VOCAB = 32000
WIDTH = 4096
SLICE = 125
LANES = 128
SCALE = 32768.0 / SAMPLES
Z_FAR_FIRST = (4, 3, 5, 2, 6, 1, 7)
NEIGHBOURS = (2, 1, 3, 0)
FAR_FIRST = (10, 6, 9, 11, 14, 2, 8, 5, 7, 13, 15, 1, 3, 4, 12)
STEP_COLUMNS = 512
STEPS = tuple(-(-min(4000 * (k + 1) + LANES, VOCAB) // STEP_COLUMNS) for k in range(8))
PARTS = 8
WINDOW = 17
LAG = 4
ITEMS = ((0, 2), (2, 1), (3, 1))
DIRECT = 1
ALONG_Z = 4 - DIRECT
LOW = -3.0e38


def remote(src, dst, send_sem, recv_sem, hst, loc):
    return pltpu.make_async_remote_copy(
        src_ref=src,
        dst_ref=dst,
        send_sem=send_sem,
        recv_sem=recv_sem,
        device_id={"hst": hst, "local": loc},
        device_id_type=MESH,
    )


def lane_index(rows):
    return lax.broadcasted_iota(jnp.int32, (rows, LANES), 1)


def masked_top(values):
    return jnp.max(
        jnp.where(lane_index(SAMPLES) < SLICE, values, LOW), axis=1, keepdims=True
    )


def masked_weights(values, top):
    valid = lane_index(SAMPLES) < SLICE
    weights = jnp.where(valid, jnp.exp(values - top), 0.0)
    return split_two(weights), jnp.sum(weights, axis=1, keepdims=True)


def product_with(weights, rows):
    product = lax.dot_general(
        weights, rows, (((1,), (1,)), ((), ())), preferred_element_type=F32
    )
    return product[:SAMPLES] + product[SAMPLES:]


def packed_stats(top, total):
    lane = lane_index(8)
    tile = jnp.zeros((8, LANES), F32)
    for r in range(3):
        tile = jnp.where((lane >= 16 * r) & (lane < 16 * r + 16), top[8 * r : 8 * r + 8], tile)
        low = 48 + 16 * r
        tile = jnp.where((lane >= low) & (lane < low + 16), total[8 * r : 8 * r + 8], tile)
    return tile


def split_two(weights):
    high = weights.astype(BF16)
    low = (weights - high.astype(F32)).astype(BF16)
    return jnp.concatenate([high, low], axis=0)[:, :SLICE]


def own_part(own, rows, out):
    top = masked_top(own)
    weights, total = masked_weights(own, top)
    product = product_with(weights, rows)
    for b in range(16):
        out[b, 0:SAMPLES, :] = product[:, LANES * b : LANES * (b + 1)]
    return top, total


def other_part(top, total, other, rows, out, y, finished):
    joined = jnp.maximum(top, masked_top(other))
    weights, more = masked_weights(other, joined)
    scale = jnp.exp(top - joined)
    stats = packed_stats(joined, total * scale + more)
    for dy in NEIGHBOURS:
        to_y = (y + dy) % 4
        product = product_with(
            weights, rows[pl.ds(pl.multiple_of(to_y * 4 * LANES, 4 * LANES), 4 * LANES), :]
        )
        for n in range(4):
            b = 4 * to_y + n
            out[b, 0:SAMPLES, :] = (
                out[b, 0:SAMPLES, :] * scale + product[:, LANES * n : LANES * (n + 1)]
            )
            out[b, SAMPLES:32, :] = stats
        finished(dy, to_y)


def factors(stat, joined):
    scale = jnp.exp(stat - joined)
    return scale, [scale[:, 16 * r : 16 * r + 1] for r in range(3)]


def join_plane(own, here, came):
    mine = own[here]
    stats = [mine[SAMPLES:32]] + [came[k, SAMPLES:32, :] for k in range(15)]
    joined = stats[0]
    for stat in stats[1:]:
        joined = jnp.maximum(joined, stat)
    total = jnp.zeros((8, LANES), F32)
    sums = [jnp.zeros((8, LANES), F32) for _ in range(3)]
    for k in range(16):
        scale, rows = factors(stats[k], joined)
        total = total + stats[k] * pltpu.roll(scale, 48, 1)
        for r in range(3):
            block = mine[8 * r : 8 * r + 8] if k == 0 else came[k - 1, 8 * r : 8 * r + 8, :]
            sums[r] = sums[r] + block * rows[r]
    tops = [joined[:, 16 * r : 16 * r + 1] for r in range(3)]
    totals = [total[:, 48 + 16 * r : 49 + 16 * r] for r in range(3)]
    return sums, tops, totals


def kernel(
    counts_hbm, ids_hbm, logits_hbm, hidden_hbm, weight_hbm, perm_hbm,
    grad_ref, hidden_out,
    counts, ids, x_in, local, hidden, weight, w_perm,
    count_to, count_from, blocks, from_core,
    got1, second, got2, third, from_z, c_from, c_sum, c_got,
    t_own, t_plane, s_own, s_plane, w_to, w_from, w_other,
    z_to, z_from, teacher, student, s_other, t_other,
    load_sems, core_recv, ring_recv, cross_recv, many_recv, send_sems,
):
    hst, loc = lax.axis_index("hst"), lax.axis_index("local")
    z, c = hst // 2, hst % 2
    y, x = loc // 4, loc % 4
    other = z * 2 + (1 - c)

    early = [
        pltpu.make_async_copy(ids_hbm, ids, load_sems.at[PARTS]),
        pltpu.make_async_copy(counts_hbm, counts, load_sems.at[PARTS + 1]),
    ]
    loads = [
        pltpu.make_async_copy(
            logits_hbm.at[:, pl.ds(low, high - low)], x_in.at[:, pl.ds(low, high - low)],
            load_sems.at[k],
        )
        for k, (low, high) in enumerate(
            (STEP_COLUMNS * ((0,) + STEPS)[k], min(STEP_COLUMNS * STEPS[k], VOCAB))
            for k in range(PARTS)
        )
    ]
    for load in early + loads[:1]:
        load.start()

    barrier = pltpu.get_barrier_semaphore()

    def greet(to_hst, to_loc):
        pl.semaphore_signal(
            barrier, inc=1, device_id={"hst": to_hst, "local": to_loc}, device_id_type=MESH
        )

    for k in range(1, 8):
        greet(((z + k) % 8) * 2 + c, loc)
    for k in FAR_FIRST:
        greet(hst, ((y + k // 4) % 4) * 4 + (x + k % 4) % 4)
    greet(other, loc)

    for load in loads[1:]:
        load.start()
    late = [
        pltpu.make_async_copy(hidden_hbm, hidden, load_sems.at[PARTS + 2]),
        pltpu.make_async_copy(weight_hbm, weight, load_sems.at[PARTS + 3]),
    ]
    for load in late:
        load.start()
    for a in range(8):
        for b in range(2):
            pltpu.make_async_copy(
                perm_hbm.at[a, b], w_perm.at[b, :, :, a], load_sems.at[PARTS + 4]
            ).start()
    late.append(pltpu.make_async_copy(w_perm, w_perm, load_sems.at[PARTS + 4]))
    for load in early:
        load.wait()

    place = lax.broadcasted_iota(jnp.int32, (SAMPLES, SAMPLES), 0)
    highs, lows = [], []
    for client in range(2):
        chosen = ids[client : client + 1, :] == place
        high = (counts[client] // 256) * 256
        highs.append(jnp.where(chosen, high.astype(F32), 0.0))
        lows.append(jnp.where(chosen, (counts[client] - high).astype(F32), 0.0))
    one = jnp.concatenate(highs + lows, axis=1)
    none = jnp.zeros_like(one)
    selector = jnp.concatenate(
        [jnp.concatenate([one, none], axis=1), jnp.concatenate([none, one], axis=1)], axis=0
    ).astype(BF16)
    count_sum = (counts[0] + counts[1]).astype(F32)
    count_to[...] = jnp.full((8, LANES), count_sum, F32)
    local[VOCAB // LANES] = jnp.zeros((SAMPLES, LANES), F32)
    lane = lane_index(SAMPLES)
    valid = lane < SLICE

    def multiply(step):
        at = step * STEP_COLUMNS
        groups = min(2, (VOCAB - at) // 256)
        columns = [x_in[:, at + 256 * g : at + 256 * (g + 1)] for g in range(groups)]
        stacked = jnp.concatenate([part for part in columns for _ in range(2)], axis=0)
        sums = jnp.dot(
            selector[: 24 * groups, : 96 * groups], stacked, preferred_element_type=F32
        )
        for g in range(groups):
            tile = at // LANES + 2 * g
            local[tile] = sums[24 * g : 24 * g + 24, :LANES]
            local[tile + 1] = sums[24 * g : 24 * g + 24, LANES:]

    places = []
    for color in range(2):
        for k in range(16):
            dx, dy = (k + 4 - x) % 4, (k // 4 + 4 - y) % 4
            along, across = (dy, dx) if color else (dx, dy)
            places.append(along * 4 + across)

    def first_tile(k, side):
        return (32 * k + 16 * side) * SLICE // LANES

    along_x = [y * 4 + (x + n) % 4 for n in range(4)]
    along_y = [((y + n) % 4) * 4 + x for n in range(4)]
    ways = (along_x, along_y)
    core_copies = []

    def send(src, dst, sem, recv_sem, to_hst, to_loc):
        copy = remote(src, dst, send_sems.at[sem], recv_sem, to_hst, to_loc)
        copy.start()
        return copy

    def arrived(ref, recv_sem):
        pltpu.make_async_copy(ref, ref, recv_sem).wait()

    def group(k, n, low=0, count=4):
        return blocks.at[pl.ds(16 * k + 4 * n + low, count)]

    def receive_core(k):
        core_copies[k].wait_recv()
        counted = count_from[0:1, :] + count_sum
        for side_c in range(2):

            @pl.when(c == side_c)
            def cut(side_c=side_c):
                base = first_tile(k, side_c)
                for n in range(16):
                    begin = (32 * k + 16 * side_c + n) * SLICE
                    tile, shift = begin // LANES, begin % LANES
                    block = local[tile] + from_core[k, tile - base]
                    if shift + SLICE > LANES:
                        after = local[tile + 1] + from_core[k, tile + 1 - base]
                        block = jnp.where(lane >= shift, block, after)
                    if shift:
                        block = pltpu.roll(block, LANES - shift, 1)
                    blocks[16 * k + places[16 * (k % 2) + n]] = jnp.where(valid, block, counted)


        @pl.when(z != k)
        def along_z():
            came_from = (k + 8 - z) % 8
            send(
                group(k, 2, DIRECT, ALONG_Z), c_from.at[came_from - 1], 11, many_recv.at[8],
                2 * k + c, loc,
            )

        way = ways[k % 2]
        if DIRECT:
            send(
                group(k, 2, 0, DIRECT), got1.at[k, pl.ds(8, DIRECT)], 1, ring_recv.at[max(0, k // 2 - 1)],
                hst, way[2],
            )
        send(group(k, 1), got1.at[k, pl.ds(0, 4)], 1, ring_recv.at[max(0, k // 2 - 1)], hst, way[1])
        send(group(k, 3), got1.at[k, pl.ds(4, 4)], 1, ring_recv.at[max(0, k // 2 - 1)], hst, way[3])

    for k in range(8):
        loads[k].wait()
        for step in range(((0,) + STEPS)[k], STEPS[k]):
            multiply(step)
        if k == 0:
            pl.semaphore_wait(barrier, 23)
            count_copy = send(count_to, count_from, 9, many_recv.at[6], other, loc)
        window = c * first_tile(k, 0) + (1 - c) * first_tile(k, 1)
        core_copies.append(
            send(
                local.at[pl.ds(window, WINDOW)], from_core.at[k], 0, core_recv.at[k], other, loc
            )
        )
        if k >= LAG:
            if k == LAG:
                count_copy.wait_recv()
            receive_core(k - LAG)
    for k in range(8 - LAG, 8):
        receive_core(k)
    for load in late:
        load.wait()

    @pl.when(c == 0)
    def widen_second():
        w_to[...] = w_perm[1].reshape(WIDTH // 2, SLICE).astype(F32)

    @pl.when(c == 1)
    def widen_first():
        w_to[...] = w_perm[0].reshape(WIDTH // 2, SLICE).astype(F32)

    w_copy = send(w_to, w_from, 5, many_recv.at[0], other, loc)
    student[:, :SLICE] = jnp.dot(hidden[...], weight[...], preferred_element_type=F32)
    student[:, SLICE:] = jnp.zeros((SAMPLES, LANES - SLICE), F32)
    s_copy = send(student, s_other, 7, many_recv.at[1], other, loc)
    w_copy.wait_recv()
    w_other[...] = w_from[...].astype(BF16)
    s_copy.wait_recv()
    own_rows = w_perm[c].reshape(WIDTH // 2, SLICE)
    top, total = own_part(student[...], own_rows, s_own)
    other_part(top, total, s_other[...], w_other, s_own, y, lambda dy, to_y: None)

    for part, (first_item, items) in enumerate(ITEMS):
        arrived(got1.at[pl.ds(2 * first_item, 2 * items)], ring_recv.at[part])
        for k in range(2 * first_item, 2 * (first_item + items)):
            for n in range(4):
                total = blocks[16 * k + n] + (got1[k, n] + got1[k, 4 + n])
                if n < DIRECT:
                    total = total + got1[k, 8 + n]
                second[k % 2, n, k // 2] = total
        taken = pl.ds(first_item, items)
        for n in (2, 1, 3):
            for color in range(2):
                send(
                    second.at[color, n, taken], got2.at[color, n - 1, taken], 2,
                    cross_recv.at[part], hst, ways[1 - color][n],
                )
    arrived(c_from, many_recv.at[8])
    odd = z % 2
    for n in range(ALONG_Z):
        at = 16 * z + 8 + DIRECT + n
        total = blocks[at]
        for k in range(7):
            total = total + c_from[k, n]
        c_sum[n] = total
        across = DIRECT + n
        to_x = (x + 2 * (1 - odd) + across * odd) % 4
        to_y = (y + 2 * odd + across * (1 - odd)) % 4
        send(c_sum.at[n], c_got.at[n], 12, many_recv.at[9], hst, to_y * 4 + to_x)
    for part, (first_item, items) in enumerate(ITEMS):
        arrived(got2.at[:, :, pl.ds(first_item, items)], cross_recv.at[part])
        for item in range(first_item, first_item + items):
            for color in range(2):
                third[2 * item + color] = (second[color, 0, item] + got2[color, 0, item]) + (
                    got2[color, 1, item] + got2[color, 2, item]
                )
        for n in range(2 * items):
            to_z = 2 * first_item + (z + 1 + n) % (2 * items)

            @pl.when(z != to_z)
            def to_owner(to_z=to_z):
                slot = (to_z + 8 - z) % 8 - 1
                send(third.at[to_z], from_z.at[slot], 3, many_recv.at[2], 2 * to_z + c, loc)

    def plane(src, dst, sem, recv_sem):
        for k in FAR_FIRST:
            to = ((y + k // 4) % 4) * 4 + (x + k % 4) % 4
            send(src.at[to], dst.at[k - 1], sem, recv_sem, hst, to)

    plane(s_own, s_plane, 6, many_recv.at[3])
    arrived(from_z, many_recv.at[2])
    summed = third[z]
    for k in range(7):
        summed = summed + from_z[k]
    arrived(c_got, many_recv.at[9])
    for n in range(ALONG_Z):
        summed = summed + c_got[n]

    ensemble = summed / summed[:, SLICE : SLICE + 1]
    teacher[...] = ensemble
    t_copy = send(teacher, t_other, 10, many_recv.at[7], other, loc)
    top, total = own_part(ensemble, own_rows, t_own)
    t_copy.wait_recv()
    def send_row(dy, to_y):
        for dx in NEIGHBOURS:
            k = 4 * dy + dx
            if k:
                to = to_y * 4 + (x + dx) % 4
                send(t_own.at[to], t_plane.at[k - 1], 8, many_recv.at[4], hst, to)

    other_part(top, total, t_other[...], w_other, t_own, y, send_row)
    arrived(s_plane, many_recv.at[3])
    s_sums, s_tops, s_totals = join_plane(s_own, loc, s_plane)
    lane8 = lane_index(8)

    def spread(sums, tops, totals, base, tile, tops_tile):
        for r in range(3):
            low = base + 20 * r
            inside = (lane8 >= low) & (lane8 < low + 16)
            ending = (lane8 >= low + 16) & (lane8 < low + 20)
            for k in range(8):
                moved = pltpu.roll(sums[r], (low - 16 * k) % LANES, 1)
                tile[k] = jnp.where(ending, totals[r], jnp.where(inside, moved, tile[k]))
            tops_tile = jnp.where(inside | ending, tops[r], tops_tile)
        return tops_tile

    tiles = [jnp.zeros((8, LANES), F32) for _ in range(8)]
    tops_tile = spread(s_sums, s_tops, s_totals, 60, tiles, jnp.zeros((8, LANES), F32))
    arrived(t_plane, many_recv.at[4])
    t_sums, t_tops, t_totals = join_plane(t_own, loc, t_plane)
    tops_tile = spread(t_sums, t_tops, t_totals, 0, tiles, tops_tile)
    for k in range(8):
        z_to[k, 0:8, :] = tiles[k]
        z_to[k, 8:16, :] = tops_tile
    for k in Z_FAR_FIRST:
        to_z = (z + k) % 8
        send(z_to.at[to_z], z_from.at[k - 1], 4, many_recv.at[5], to_z * 2 + c, loc)
    arrived(z_from, many_recv.at[5])
    mine = z_to[z]
    pieces = [mine] + [z_from[k] for k in range(7)]
    joined = pieces[0][8:16]
    for piece in pieces[1:]:
        joined = jnp.maximum(joined, piece[8:16])
    sums = jnp.zeros((8, LANES), F32)
    for piece in pieces:
        sums = sums + piece[0:8] * jnp.exp(piece[8:16] - joined)

    for r in range(3):
        t_low, s_low = 20 * r, 60 + 20 * r
        t_top, s_top = joined[:, t_low : t_low + 1], joined[:, s_low : s_low + 1]
        t_total = sums[:, t_low + 16 : t_low + 17]
        s_total = sums[:, s_low + 16 : s_low + 17]
        rows = slice(8 * r, 8 * r + 8)
        t_part = pltpu.roll(sums, (LANES - t_low) % LANES, 1) / t_total
        s_part = pltpu.roll(sums, (LANES - s_low) % LANES, 1) / s_total
        hidden_out[rows, :] = (SCALE * (s_part - t_part))[:, :16]
        s_prob = jnp.exp(student[rows, :] - s_top) / s_total
        t_prob = jnp.exp(teacher[rows, :] - t_top) / t_total
        grad_ref[rows, :] = (SCALE * (s_prob - t_prob))[:, :SLICE]

    for n, ref in enumerate(
        (from_core, got1, got2, from_z, z_from, w_to, s_plane, student, t_plane, count_to, teacher, c_from, c_got)
    ):
        arrived(ref, send_sems.at[n])


def finish(grad, grad_hidden, hidden, weight_out, hidden_out, rows, sems):
    rounded = grad[...].astype(BF16)
    size = WIDTH // 4
    copies = []
    for k in range(4):
        part = pl.ds(k * size, size)
        rows[part, :] = lax.dot_general(
            hidden[:, part], rounded, (((0,), (0,)), ((), ())), preferred_element_type=F32
        ).astype(BF16)
        copies.append(pltpu.make_async_copy(rows.at[part], weight_out.at[part], sems.at[k]))
        copies[k].start()
    hidden_out[...] = grad_hidden[...].T
    for copy in copies:
        copy.wait()


def per_device(teacher_logits, sample_ids, client_counts, student_hidden, student_weight):
    logits = teacher_logits.reshape(2 * SAMPLES, VOCAB)
    perm = student_weight.reshape(8, 2, 4, 4, 16, SLICE)
    any_spec = pl.BlockSpec(memory_space=pltpu.HBM)
    vmem = pl.BlockSpec(memory_space=pltpu.VMEM)
    block = (SAMPLES, LANES)
    tall = (16, 32, LANES)
    dma = pltpu.SemaphoreType.DMA
    grad, grad_hidden = pl.pallas_call(
        kernel,
        out_shape=(
            pltpu.VMEM((SAMPLES, SLICE), F32),
            pltpu.VMEM((SAMPLES, 16), F32),
        ),
        in_specs=[any_spec] * 6,
        out_specs=(vmem, vmem),
        scratch_shapes=[
            pltpu.SMEM((2,), jnp.int32),
            pltpu.VMEM((2, SAMPLES), jnp.int32),
            pltpu.VMEM((2 * SAMPLES, VOCAB), BF16),
            pltpu.VMEM((VOCAB // LANES + 2, *block), F32),
            pltpu.VMEM((SAMPLES, WIDTH), BF16),
            pltpu.VMEM((WIDTH, SLICE), BF16),
            pltpu.VMEM((2, 4, 4, 8, 16, SLICE), BF16),
            pltpu.VMEM((8, LANES), F32),
            pltpu.VMEM((8, LANES), F32),
            pltpu.VMEM((128, *block), F32),
            pltpu.VMEM((8, WINDOW, *block), F32),
            pltpu.VMEM((8, 8 + DIRECT, *block), F32),
            pltpu.VMEM((2, 4, 4, *block), F32),
            pltpu.VMEM((2, 3, 4, *block), F32),
            pltpu.VMEM((8, *block), F32),
            pltpu.VMEM((7, *block), F32),
            pltpu.VMEM((7, ALONG_Z, *block), F32),
            pltpu.VMEM((ALONG_Z, *block), F32),
            pltpu.VMEM((ALONG_Z, *block), F32),
            pltpu.VMEM(tall, F32),
            pltpu.VMEM((15, 32, LANES), F32),
            pltpu.VMEM(tall, F32),
            pltpu.VMEM((15, 32, LANES), F32),
            pltpu.VMEM((WIDTH // 2, SLICE), F32),
            pltpu.VMEM((WIDTH // 2, SLICE), F32),
            pltpu.VMEM((WIDTH // 2, SLICE), BF16),
            pltpu.VMEM((8, 16, LANES), F32),
            pltpu.VMEM((7, 16, LANES), F32),
            pltpu.VMEM(block, F32),
            pltpu.VMEM(block, F32),
            pltpu.VMEM(block, F32),
            pltpu.VMEM(block, F32),
            dma((PARTS + 5,)),
            dma((8,)),
            dma((3,)),
            dma((3,)),
            dma((10,)),
            dma((13,)),
        ],
        compiler_params=pltpu.CompilerParams(
            collective_id=0, has_side_effects=True, vmem_limit_bytes=63 * 1024 * 1024
        ),
        name="distill",
    )(client_counts, sample_ids, logits, student_hidden, student_weight, perm)
    grad_weight, turned = pl.pallas_call(
        finish,
        out_shape=(
            jax.ShapeDtypeStruct((WIDTH, SLICE), BF16),
            jax.ShapeDtypeStruct((16, SAMPLES), F32),
        ),
        in_specs=[vmem] * 3,
        out_specs=(any_spec, vmem),
        scratch_shapes=[pltpu.VMEM((WIDTH, SLICE), BF16), dma((4,))],
        compiler_params=pltpu.CompilerParams(vmem_limit_bytes=8 * 1024 * 1024),
        name="finish",
    )(grad, grad_hidden, student_hidden)
    return grad_weight, turned.T


def solution(mesh):
    both = ("hst", "local")
    return jax.shard_map(
        per_device,
        mesh=mesh,
        in_specs=(P(both, None, None), P(both, None), P(both), P(), P(None, both)),
        out_specs=(P(None, both), P(None, both)),
        check_vma=False,
    )
```

```python
import jax
import jax.numpy as jnp
from jax import lax
from jax.experimental import pallas as pl
from jax.experimental.pallas import tpu as pltpu
from jax.sharding import PartitionSpec as P

MESH = pl.DeviceIdType.MESH
F32 = jnp.float32
BF16 = jnp.bfloat16
SAMPLES = 24
VOCAB = 32000
WIDTH = 4096
SLICE = 125
LANES = 128
SCALE = 32768.0 / SAMPLES
Z_FAR_FIRST = (4, 3, 5, 2, 6, 1, 7)
NEIGHBOURS = (2, 1, 3, 0)
FAR_FIRST = (10, 6, 9, 11, 14, 2, 8, 5, 7, 13, 15, 1, 3, 4, 12)
STEP_COLUMNS = 512
STEPS = tuple(-(-min(4000 * (k + 1) + LANES, VOCAB) // STEP_COLUMNS) for k in range(8))
PARTS = 8
WINDOW = 17
LAG = 4
ITEMS = ((0, 2), (2, 1), (3, 1))
DIRECT = 1
ALONG_Z = 4 - DIRECT
LOW = -3.0e38


def remote(src, dst, send_sem, recv_sem, hst, loc):
    return pltpu.make_async_remote_copy(
        src_ref=src,
        dst_ref=dst,
        send_sem=send_sem,
        recv_sem=recv_sem,
        device_id={"hst": hst, "local": loc},
        device_id_type=MESH,
    )


def lane_index(rows):
    return lax.broadcasted_iota(jnp.int32, (rows, LANES), 1)


def masked_top(values):
    return jnp.max(
        jnp.where(lane_index(SAMPLES) < SLICE, values, LOW), axis=1, keepdims=True
    )


def masked_weights(values, top):
    valid = lane_index(SAMPLES) < SLICE
    weights = jnp.where(valid, jnp.exp(values - top), 0.0)
    return split_two(weights), jnp.sum(weights, axis=1, keepdims=True)


def product_with(weights, rows):
    product = lax.dot_general(
        weights, rows, (((1,), (1,)), ((), ())), preferred_element_type=F32
    )
    return product[:SAMPLES] + product[SAMPLES:]


def packed_stats(top, total):
    lane = lane_index(8)
    tile = jnp.zeros((8, LANES), F32)
    for r in range(3):
        tile = jnp.where((lane >= 16 * r) & (lane < 16 * r + 16), top[8 * r : 8 * r + 8], tile)
        low = 48 + 16 * r
        tile = jnp.where((lane >= low) & (lane < low + 16), total[8 * r : 8 * r + 8], tile)
    return tile


def split_two(weights):
    high = weights.astype(BF16)
    low = (weights - high.astype(F32)).astype(BF16)
    return jnp.concatenate([high, low], axis=0)[:, :SLICE]


def own_part(own, rows, out):
    top = masked_top(own)
    weights, total = masked_weights(own, top)
    product = product_with(weights, rows)
    for b in range(16):
        out[b, 0:SAMPLES, :] = product[:, LANES * b : LANES * (b + 1)]
    return top, total


def other_part(top, total, other, rows, out, y, finished):
    joined = jnp.maximum(top, masked_top(other))
    weights, more = masked_weights(other, joined)
    scale = jnp.exp(top - joined)
    stats = packed_stats(joined, total * scale + more)
    for dy in NEIGHBOURS:
        to_y = (y + dy) % 4
        product = product_with(
            weights, rows[pl.ds(pl.multiple_of(to_y * 4 * LANES, 4 * LANES), 4 * LANES), :]
        )
        for n in range(4):
            b = 4 * to_y + n
            out[b, 0:SAMPLES, :] = (
                out[b, 0:SAMPLES, :] * scale + product[:, LANES * n : LANES * (n + 1)]
            )
            out[b, SAMPLES:32, :] = stats
        finished(dy, to_y)


def factors(stat, joined):
    scale = jnp.exp(stat - joined)
    return scale, [scale[:, 16 * r : 16 * r + 1] for r in range(3)]


def join_plane(own, here, came):
    mine = own[here]
    stats = [mine[SAMPLES:32]] + [came[k, SAMPLES:32, :] for k in range(15)]
    joined = stats[0]
    for stat in stats[1:]:
        joined = jnp.maximum(joined, stat)
    total = jnp.zeros((8, LANES), F32)
    sums = [jnp.zeros((8, LANES), F32) for _ in range(3)]
    for k in range(16):
        scale, rows = factors(stats[k], joined)
        total = total + stats[k] * pltpu.roll(scale, 48, 1)
        for r in range(3):
            block = mine[8 * r : 8 * r + 8] if k == 0 else came[k - 1, 8 * r : 8 * r + 8, :]
            sums[r] = sums[r] + block * rows[r]
    tops = [joined[:, 16 * r : 16 * r + 1] for r in range(3)]
    totals = [total[:, 48 + 16 * r : 49 + 16 * r] for r in range(3)]
    return sums, tops, totals


def kernel(
    counts_hbm, ids_hbm, logits_hbm, hidden_hbm, weight_hbm, perm_hbm,
    grad_ref, hidden_out,
    counts, ids, x_in, local, hidden, weight, w_perm,
    count_to, count_from, blocks, from_core,
    got1, second, got2, third, from_z, c_from, c_sum, c_got,
    t_own, t_plane, s_own, s_plane, w_to, w_from, w_other,
    z_to, z_from, teacher, student, s_other, t_other,
    load_sems, core_recv, ring_recv, cross_recv, many_recv, send_sems,
):
    hst, loc = lax.axis_index("hst"), lax.axis_index("local")
    z, c = hst // 2, hst % 2
    y, x = loc // 4, loc % 4
    other = z * 2 + (1 - c)

    early = [
        pltpu.make_async_copy(ids_hbm, ids, load_sems.at[PARTS]),
        pltpu.make_async_copy(counts_hbm, counts, load_sems.at[PARTS + 1]),
    ]
    loads = [
        pltpu.make_async_copy(
            logits_hbm.at[:, pl.ds(low, high - low)], x_in.at[:, pl.ds(low, high - low)],
            load_sems.at[k],
        )
        for k, (low, high) in enumerate(
            (STEP_COLUMNS * ((0,) + STEPS)[k], min(STEP_COLUMNS * STEPS[k], VOCAB))
            for k in range(PARTS)
        )
    ]
    for load in early + loads[:1]:
        load.start()

    barrier = pltpu.get_barrier_semaphore()

    def greet(to_hst, to_loc):
        pl.semaphore_signal(
            barrier, inc=1, device_id={"hst": to_hst, "local": to_loc}, device_id_type=MESH
        )

    for k in range(1, 8):
        greet(((z + k) % 8) * 2 + c, loc)
    for k in FAR_FIRST:
        greet(hst, ((y + k // 4) % 4) * 4 + (x + k % 4) % 4)
    greet(other, loc)

    for load in loads[1:]:
        load.start()
    late = [
        pltpu.make_async_copy(hidden_hbm, hidden, load_sems.at[PARTS + 2]),
        pltpu.make_async_copy(weight_hbm, weight, load_sems.at[PARTS + 3]),
    ]
    for load in late:
        load.start()
    for a in range(8):
        for b in range(2):
            pltpu.make_async_copy(
                perm_hbm.at[a, b], w_perm.at[b, :, :, a], load_sems.at[PARTS + 4]
            ).start()
    late.append(pltpu.make_async_copy(w_perm, w_perm, load_sems.at[PARTS + 4]))
    for load in early:
        load.wait()

    place = lax.broadcasted_iota(jnp.int32, (SAMPLES, SAMPLES), 0)
    highs, lows = [], []
    for client in range(2):
        chosen = ids[client : client + 1, :] == place
        high = (counts[client] // 256) * 256
        highs.append(jnp.where(chosen, high.astype(F32), 0.0))
        lows.append(jnp.where(chosen, (counts[client] - high).astype(F32), 0.0))
    one = jnp.concatenate(highs + lows, axis=1)
    none = jnp.zeros_like(one)
    selector = jnp.concatenate(
        [jnp.concatenate([one, none], axis=1), jnp.concatenate([none, one], axis=1)], axis=0
    ).astype(BF16)
    count_sum = (counts[0] + counts[1]).astype(F32)
    count_to[...] = jnp.full((8, LANES), count_sum, F32)
    local[VOCAB // LANES] = jnp.zeros((SAMPLES, LANES), F32)
    lane = lane_index(SAMPLES)
    valid = lane < SLICE

    def multiply(step):
        at = step * STEP_COLUMNS
        groups = min(2, (VOCAB - at) // 256)
        columns = [x_in[:, at + 256 * g : at + 256 * (g + 1)] for g in range(groups)]
        stacked = jnp.concatenate([part for part in columns for _ in range(2)], axis=0)
        sums = jnp.dot(
            selector[: 24 * groups, : 96 * groups], stacked, preferred_element_type=F32
        )
        for g in range(groups):
            tile = at // LANES + 2 * g
            local[tile] = sums[24 * g : 24 * g + 24, :LANES]
            local[tile + 1] = sums[24 * g : 24 * g + 24, LANES:]

    places = []
    for color in range(2):
        for k in range(16):
            dx, dy = (k + 4 - x) % 4, (k // 4 + 4 - y) % 4
            along, across = (dy, dx) if color else (dx, dy)
            places.append(along * 4 + across)

    def first_tile(k, side):
        return (32 * k + 16 * side) * SLICE // LANES

    along_x = [y * 4 + (x + n) % 4 for n in range(4)]
    along_y = [((y + n) % 4) * 4 + x for n in range(4)]
    ways = (along_x, along_y)
    core_copies = []

    def send(src, dst, sem, recv_sem, to_hst, to_loc):
        copy = remote(src, dst, send_sems.at[sem], recv_sem, to_hst, to_loc)
        copy.start()
        return copy

    def arrived(ref, recv_sem):
        pltpu.make_async_copy(ref, ref, recv_sem).wait()

    def group(k, n, low=0, count=4):
        return blocks.at[pl.ds(16 * k + 4 * n + low, count)]

    def receive_core(k):
        core_copies[k].wait_recv()
        counted = count_from[0:1, :] + count_sum
        for side_c in range(2):

            @pl.when(c == side_c)
            def cut(side_c=side_c):
                base = first_tile(k, side_c)
                for n in range(16):
                    begin = (32 * k + 16 * side_c + n) * SLICE
                    tile, shift = begin // LANES, begin % LANES
                    block = local[tile] + from_core[k, tile - base]
                    if shift + SLICE > LANES:
                        after = local[tile + 1] + from_core[k, tile + 1 - base]
                        block = jnp.where(lane >= shift, block, after)
                    if shift:
                        block = pltpu.roll(block, LANES - shift, 1)
                    blocks[16 * k + places[16 * (k % 2) + n]] = jnp.where(valid, block, counted)


        @pl.when(z != k)
        def along_z():
            came_from = (k + 8 - z) % 8
            send(
                group(k, 2, DIRECT, ALONG_Z), c_from.at[came_from - 1], 11, many_recv.at[8],
                2 * k + c, loc,
            )

        way = ways[k % 2]
        if DIRECT:
            send(
                group(k, 2, 0, DIRECT), got1.at[k, pl.ds(8, DIRECT)], 1, ring_recv.at[max(0, k // 2 - 1)],
                hst, way[2],
            )
        send(group(k, 1), got1.at[k, pl.ds(0, 4)], 1, ring_recv.at[max(0, k // 2 - 1)], hst, way[1])
        send(group(k, 3), got1.at[k, pl.ds(4, 4)], 1, ring_recv.at[max(0, k // 2 - 1)], hst, way[3])

    for k in range(8):
        loads[k].wait()
        for step in range(((0,) + STEPS)[k], STEPS[k]):
            multiply(step)
        if k == 0:
            pl.semaphore_wait(barrier, 23)
            count_copy = send(count_to, count_from, 9, many_recv.at[6], other, loc)
        window = c * first_tile(k, 0) + (1 - c) * first_tile(k, 1)
        core_copies.append(
            send(
                local.at[pl.ds(window, WINDOW)], from_core.at[k], 0, core_recv.at[k], other, loc
            )
        )
        if k >= LAG:
            if k == LAG:
                count_copy.wait_recv()
            receive_core(k - LAG)
    for k in range(8 - LAG, 8):
        receive_core(k)
    for load in late:
        load.wait()

    @pl.when(c == 0)
    def widen_second():
        w_to[...] = w_perm[1].reshape(WIDTH // 2, SLICE).astype(F32)

    @pl.when(c == 1)
    def widen_first():
        w_to[...] = w_perm[0].reshape(WIDTH // 2, SLICE).astype(F32)

    w_copy = send(w_to, w_from, 5, many_recv.at[0], other, loc)
    student[:, :SLICE] = jnp.dot(hidden[...], weight[...], preferred_element_type=F32)
    student[:, SLICE:] = jnp.zeros((SAMPLES, LANES - SLICE), F32)
    s_copy = send(student, s_other, 7, many_recv.at[1], other, loc)
    w_copy.wait_recv()
    w_other[...] = w_from[...].astype(BF16)
    s_copy.wait_recv()
    own_rows = w_perm[c].reshape(WIDTH // 2, SLICE)
    top, total = own_part(student[...], own_rows, s_own)
    other_part(top, total, s_other[...], w_other, s_own, y, lambda dy, to_y: None)

    for part, (first_item, items) in enumerate(ITEMS):
        arrived(got1.at[pl.ds(2 * first_item, 2 * items)], ring_recv.at[part])
        for k in range(2 * first_item, 2 * (first_item + items)):
            for n in range(4):
                total = blocks[16 * k + n] + (got1[k, n] + got1[k, 4 + n])
                if n < DIRECT:
                    total = total + got1[k, 8 + n]
                second[k % 2, n, k // 2] = total
        taken = pl.ds(first_item, items)
        for n in (2, 1, 3):
            for color in range(2):
                send(
                    second.at[color, n, taken], got2.at[color, n - 1, taken], 2,
                    cross_recv.at[part], hst, ways[1 - color][n],
                )
    def sum_far_blocks():
        arrived(c_from, many_recv.at[8])
        odd = z % 2
        for n in range(ALONG_Z):
            at = 16 * z + 8 + DIRECT + n
            total = blocks[at]
            for k in range(7):
                total = total + c_from[k, n]
            c_sum[n] = total
            across = DIRECT + n
            to_x = (x + 2 * (1 - odd) + across * odd) % 4
            to_y = (y + 2 * odd + across * (1 - odd)) % 4
            send(c_sum.at[n], c_got.at[n], 12, many_recv.at[9], hst, to_y * 4 + to_x)

    for part, (first_item, items) in enumerate(ITEMS):
        if part == 2:
            sum_far_blocks()
        arrived(got2.at[:, :, pl.ds(first_item, items)], cross_recv.at[part])
        for item in range(first_item, first_item + items):
            for color in range(2):
                third[2 * item + color] = (second[color, 0, item] + got2[color, 0, item]) + (
                    got2[color, 1, item] + got2[color, 2, item]
                )
        for n in range(2 * items):
            to_z = 2 * first_item + (z + 1 + n) % (2 * items)

            @pl.when(z != to_z)
            def to_owner(to_z=to_z):
                slot = (to_z + 8 - z) % 8 - 1
                send(third.at[to_z], from_z.at[slot], 3, many_recv.at[2], 2 * to_z + c, loc)

    def plane(src, dst, sem, recv_sem):
        for k in FAR_FIRST:
            to = ((y + k // 4) % 4) * 4 + (x + k % 4) % 4
            send(src.at[to], dst.at[k - 1], sem, recv_sem, hst, to)

    plane(s_own, s_plane, 6, many_recv.at[3])
    arrived(from_z, many_recv.at[2])
    summed = third[z]
    for k in range(7):
        summed = summed + from_z[k]
    arrived(c_got, many_recv.at[9])
    for n in range(ALONG_Z):
        summed = summed + c_got[n]

    ensemble = summed / summed[:, SLICE : SLICE + 1]
    teacher[...] = ensemble
    t_copy = send(teacher, t_other, 10, many_recv.at[7], other, loc)
    top, total = own_part(ensemble, own_rows, t_own)
    t_copy.wait_recv()
    def send_row(dy, to_y):
        for dx in NEIGHBOURS:
            k = 4 * dy + dx
            if k:
                to = to_y * 4 + (x + dx) % 4
                send(t_own.at[to], t_plane.at[k - 1], 8, many_recv.at[4], hst, to)

    other_part(top, total, t_other[...], w_other, t_own, y, send_row)
    arrived(s_plane, many_recv.at[3])
    s_sums, s_tops, s_totals = join_plane(s_own, loc, s_plane)
    lane8 = lane_index(8)

    def spread(sums, tops, totals, base, tile, tops_tile):
        for r in range(3):
            low = base + 20 * r
            inside = (lane8 >= low) & (lane8 < low + 16)
            ending = (lane8 >= low + 16) & (lane8 < low + 20)
            for k in range(8):
                moved = pltpu.roll(sums[r], (low - 16 * k) % LANES, 1)
                tile[k] = jnp.where(ending, totals[r], jnp.where(inside, moved, tile[k]))
            tops_tile = jnp.where(inside | ending, tops[r], tops_tile)
        return tops_tile

    tiles = [jnp.zeros((8, LANES), F32) for _ in range(8)]
    tops_tile = spread(s_sums, s_tops, s_totals, 60, tiles, jnp.zeros((8, LANES), F32))
    arrived(t_plane, many_recv.at[4])
    t_sums, t_tops, t_totals = join_plane(t_own, loc, t_plane)
    tops_tile = spread(t_sums, t_tops, t_totals, 0, tiles, tops_tile)
    for k in range(8):
        z_to[k, 0:8, :] = tiles[k]
        z_to[k, 8:16, :] = tops_tile
    for k in Z_FAR_FIRST:
        to_z = (z + k) % 8
        send(z_to.at[to_z], z_from.at[k - 1], 4, many_recv.at[5], to_z * 2 + c, loc)
    arrived(z_from, many_recv.at[5])
    mine = z_to[z]
    pieces = [mine] + [z_from[k] for k in range(7)]
    joined = pieces[0][8:16]
    for piece in pieces[1:]:
        joined = jnp.maximum(joined, piece[8:16])
    sums = jnp.zeros((8, LANES), F32)
    for piece in pieces:
        sums = sums + piece[0:8] * jnp.exp(piece[8:16] - joined)

    for r in range(3):
        t_low, s_low = 20 * r, 60 + 20 * r
        t_top, s_top = joined[:, t_low : t_low + 1], joined[:, s_low : s_low + 1]
        t_total = sums[:, t_low + 16 : t_low + 17]
        s_total = sums[:, s_low + 16 : s_low + 17]
        rows = slice(8 * r, 8 * r + 8)
        t_part = pltpu.roll(sums, (LANES - t_low) % LANES, 1) / t_total
        s_part = pltpu.roll(sums, (LANES - s_low) % LANES, 1) / s_total
        hidden_out[rows, :] = (SCALE * (s_part - t_part))[:, :16]
        s_prob = jnp.exp(student[rows, :] - s_top) / s_total
        t_prob = jnp.exp(teacher[rows, :] - t_top) / t_total
        grad_ref[rows, :] = (SCALE * (s_prob - t_prob))[:, :SLICE]

    for n, ref in enumerate(
        (from_core, got1, got2, from_z, z_from, w_to, s_plane, student, t_plane, count_to, teacher, c_from, c_got)
    ):
        arrived(ref, send_sems.at[n])


def finish(grad, grad_hidden, hidden, weight_out, hidden_out, rows, sems):
    rounded = grad[...].astype(BF16)
    size = WIDTH // 4
    copies = []
    for k in range(4):
        part = pl.ds(k * size, size)
        rows[part, :] = lax.dot_general(
            hidden[:, part], rounded, (((0,), (0,)), ((), ())), preferred_element_type=F32
        ).astype(BF16)
        copies.append(pltpu.make_async_copy(rows.at[part], weight_out.at[part], sems.at[k]))
        copies[k].start()
    hidden_out[...] = grad_hidden[...].T
    for copy in copies:
        copy.wait()


def per_device(teacher_logits, sample_ids, client_counts, student_hidden, student_weight):
    logits = teacher_logits.reshape(2 * SAMPLES, VOCAB)
    perm = student_weight.reshape(8, 2, 4, 4, 16, SLICE)
    any_spec = pl.BlockSpec(memory_space=pltpu.HBM)
    vmem = pl.BlockSpec(memory_space=pltpu.VMEM)
    block = (SAMPLES, LANES)
    tall = (16, 32, LANES)
    dma = pltpu.SemaphoreType.DMA
    grad, grad_hidden = pl.pallas_call(
        kernel,
        out_shape=(
            pltpu.VMEM((SAMPLES, SLICE), F32),
            pltpu.VMEM((SAMPLES, 16), F32),
        ),
        in_specs=[any_spec] * 6,
        out_specs=(vmem, vmem),
        scratch_shapes=[
            pltpu.SMEM((2,), jnp.int32),
            pltpu.VMEM((2, SAMPLES), jnp.int32),
            pltpu.VMEM((2 * SAMPLES, VOCAB), BF16),
            pltpu.VMEM((VOCAB // LANES + 2, *block), F32),
            pltpu.VMEM((SAMPLES, WIDTH), BF16),
            pltpu.VMEM((WIDTH, SLICE), BF16),
            pltpu.VMEM((2, 4, 4, 8, 16, SLICE), BF16),
            pltpu.VMEM((8, LANES), F32),
            pltpu.VMEM((8, LANES), F32),
            pltpu.VMEM((128, *block), F32),
            pltpu.VMEM((8, WINDOW, *block), F32),
            pltpu.VMEM((8, 8 + DIRECT, *block), F32),
            pltpu.VMEM((2, 4, 4, *block), F32),
            pltpu.VMEM((2, 3, 4, *block), F32),
            pltpu.VMEM((8, *block), F32),
            pltpu.VMEM((7, *block), F32),
            pltpu.VMEM((7, ALONG_Z, *block), F32),
            pltpu.VMEM((ALONG_Z, *block), F32),
            pltpu.VMEM((ALONG_Z, *block), F32),
            pltpu.VMEM(tall, F32),
            pltpu.VMEM((15, 32, LANES), F32),
            pltpu.VMEM(tall, F32),
            pltpu.VMEM((15, 32, LANES), F32),
            pltpu.VMEM((WIDTH // 2, SLICE), F32),
            pltpu.VMEM((WIDTH // 2, SLICE), F32),
            pltpu.VMEM((WIDTH // 2, SLICE), BF16),
            pltpu.VMEM((8, 16, LANES), F32),
            pltpu.VMEM((7, 16, LANES), F32),
            pltpu.VMEM(block, F32),
            pltpu.VMEM(block, F32),
            pltpu.VMEM(block, F32),
            pltpu.VMEM(block, F32),
            dma((PARTS + 5,)),
            dma((8,)),
            dma((3,)),
            dma((3,)),
            dma((10,)),
            dma((13,)),
        ],
        compiler_params=pltpu.CompilerParams(
            collective_id=0, has_side_effects=True, vmem_limit_bytes=63 * 1024 * 1024
        ),
        name="distill",
    )(client_counts, sample_ids, logits, student_hidden, student_weight, perm)
    grad_weight, turned = pl.pallas_call(
        finish,
        out_shape=(
            jax.ShapeDtypeStruct((WIDTH, SLICE), BF16),
            jax.ShapeDtypeStruct((16, SAMPLES), F32),
        ),
        in_specs=[vmem] * 3,
        out_specs=(any_spec, vmem),
        scratch_shapes=[pltpu.VMEM((WIDTH, SLICE), BF16), dma((4,))],
        compiler_params=pltpu.CompilerParams(vmem_limit_bytes=8 * 1024 * 1024),
        name="finish",
    )(grad, grad_hidden, student_hidden)
    return grad_weight, turned.T


def solution(mesh):
    both = ("hst", "local")
    return jax.shard_map(
        per_device,
        mesh=mesh,
        in_specs=(P(both, None, None), P(both, None), P(both), P(), P(None, both)),
        out_specs=(P(None, both), P(None, both)),
        check_vma=False,
    )
```
